32 devices in a mesh: sys: 1 (over z), zdom: 4 (over y), ydom: 8 (over x, core).
Axes of the slice: x: 4, y: 4, z: 1, core: 2. Of those that a mesh axis runs over, the one named last changes fastest.
The devices are a block of a 4x4x8 slice.
Arguments:
- charge: float32 [262144], P(('sys', 'ydom', 'zdom'))
- real_mask: int32 [262144], P(('sys', 'ydom', 'zdom'))
- grid_idx: int32 [262144, 3], P(('sys', 'ydom', 'zdom'))
- spline_w: float32 [262144, 3, 4], P(('sys', 'ydom', 'zdom'))
- influence: float32 [216, 216, 216], P(('sys', 'ydom'), 'zdom')
Outputs:
- output 1: float32 [216, 216, 216], P(('sys', 'ydom'), 'zdom')
- output 2: float32 [1], P('sys')
All inputs are finite; a program needn't handle non-finite values.
Results may differ from the reference program's by a relative error of at most 0.001.
Values are sent between devices in bfloat16 or wider.
A program may use at most 768 MiB of HBM per device.

```python
import jax
import jax.numpy as jnp
from jax import lax

GRID_SIDE = 216
PER_DEV = 8192
Y_DEVS = 8
Z_DEVS = 4


def bspline_weights(frac_part):
    frac_sq = frac_part * frac_part
    frac_cube = frac_sq * frac_part
    w_zero = (1.0 - frac_part) * (1.0 - frac_part) * (1.0 - frac_part) / 6.0
    w_one = (3.0 * frac_cube - 6.0 * frac_sq + 4.0) / 6.0
    w_two = (-3.0 * frac_cube + 3.0 * frac_sq + 3.0 * frac_part + 1.0) / 6.0
    w_three = frac_cube / 6.0
    return jnp.stack([w_zero, w_one, w_two, w_three], axis=-1)


def edge_index(key, count, length):
    key_near, key_edge, key_any = jax.random.split(key, 3)
    near_edge = jax.random.randint(key_near, (count,), 0, 2)
    at_edge = length - 3 + jax.random.randint(key_edge, (count,), 0, 3)
    anywhere = jax.random.randint(key_any, (count,), 0, length)
    return jnp.where(near_edge == 1, at_edge, anywhere)


def setup_inputs(seed: int = 0, part: int = 0) -> dict:
    dev_count = Y_DEVS * Z_DEVS
    slot_count = dev_count * PER_DEV
    len_y = GRID_SIDE // Y_DEVS
    len_z = GRID_SIDE // Z_DEVS
    sub_keys = jax.random.split(jax.random.fold_in(jax.random.key(seed), part), 8)
    real_count = jax.random.randint(sub_keys[0], (dev_count, 1), PER_DEV // 8, PER_DEV + 1)
    slot_rank = jax.random.randint(sub_keys[1], (dev_count, PER_DEV), 0, PER_DEV)
    real_mask = (slot_rank < real_count).astype(jnp.int32).reshape(slot_count)
    x_idx = jax.random.randint(sub_keys[2], (slot_count,), 0, GRID_SIDE)
    y_idx = edge_index(sub_keys[3], slot_count, len_y)
    z_idx = edge_index(sub_keys[4], slot_count, len_z)
    grid_idx = jnp.stack([x_idx, y_idx, z_idx], axis=1).astype(jnp.int32)
    charge = jax.random.normal(sub_keys[5], (slot_count,), jnp.float32)
    frac_part = jax.random.uniform(sub_keys[6], (slot_count, 3), jnp.float32)
    spline_w = bspline_weights(frac_part).astype(jnp.float32)
    influence = jax.random.uniform(sub_keys[7], (GRID_SIDE, GRID_SIDE, GRID_SIDE), jnp.float32, 0.5, 1.5) * (20.0 / slot_count)
    return {'charge': charge, 'real_mask': real_mask, 'grid_idx': grid_idx, 'spline_w': spline_w, 'influence': influence}


def reference(charge, real_mask, grid_idx, spline_w, influence):
    slot_count = Y_DEVS * Z_DEVS * PER_DEV
    len_y = GRID_SIDE // Y_DEVS
    len_z = GRID_SIDE // Z_DEVS
    device = jnp.arange(slot_count) // PER_DEV
    base_x = grid_idx[:, 0]
    base_y = grid_idx[:, 1] + (device // Z_DEVS) * len_y
    base_z = grid_idx[:, 2] + (device % Z_DEVS) * len_z
    weight = charge * real_mask.astype(charge.dtype)

    def add_tap(flat_grid, tap_id):
        off_x = tap_id // 16
        off_y = (tap_id // 4) % 4
        off_z = tap_id % 4
        pos_x = (base_x + off_x) % GRID_SIDE
        pos_y = (base_y + off_y) % GRID_SIDE
        pos_z = (base_z + off_z) % GRID_SIDE
        tap_value = weight * spline_w[:, 0, off_x] * spline_w[:, 1, off_y] * spline_w[:, 2, off_z]
        flat_idx = (pos_x * GRID_SIDE + pos_y) * GRID_SIDE + pos_z
        return flat_grid.at[flat_idx].add(tap_value), None

    flat_grid = lax.scan(add_tap, jnp.zeros((GRID_SIDE * GRID_SIDE * GRID_SIDE,), charge.dtype), jnp.arange(64))[0]
    charge_grid = flat_grid.reshape(GRID_SIDE, GRID_SIDE, GRID_SIDE)
    spectrum = jnp.fft.fftn(charge_grid)
    mode_energy = 0.5 * influence * (spectrum.real * spectrum.real + spectrum.imag * spectrum.imag)
    energy = jnp.sum(mode_energy) / (GRID_SIDE * GRID_SIDE * GRID_SIDE)
    return mode_energy, jnp.reshape(energy, (1,))
```

```python
import functools
import math

import jax
import jax.numpy as jnp
import numpy as np
from jax import lax
from jax.experimental import pallas as pl
from jax.experimental.pallas import tpu as pltpu
from jax.sharding import PartitionSpec as P

MESH = pl.DeviceIdType.MESH
TAPS = 4
LANES = 128
NT_DIMS = (((1,), (1,)), ((), ()))


def round_up(value, unit):
    return -(-value // unit) * unit


def split_const(matrix):
    high = matrix.astype(jnp.bfloat16)
    low = (matrix - high.astype(np.float64)).astype(jnp.bfloat16)
    return high, low


def split_value(value):
    high = value.astype(jnp.bfloat16)
    low = (value - high.astype(jnp.float32)).astype(jnp.bfloat16)
    return high, low


def dot_f32(left, right):
    return jnp.dot(left, right, preferred_element_type=jnp.float32)


def dot_nt(left, right):
    return lax.dot_general(left, right, NT_DIMS, preferred_element_type=jnp.float32)


def spread_kernel(grid_n, rows_y, chunk, group, charge_ref, mask_ref, idx_ref, w_ref, out_ref,
                  a_hi, a_lo, b_hi, b_lo, y_ref, z_ref):
    slots = charge_ref.shape[1]
    rows_a = a_hi.shape[0]
    top_a = round_up(grid_n, 16)
    out_ref[...] = jnp.zeros_like(out_ref)
    if top_a < rows_a:
        a_hi[top_a:, :] = jnp.zeros((rows_a - top_a, chunk), jnp.bfloat16)
        a_lo[top_a:, :] = jnp.zeros((rows_a - top_a, chunk), jnp.bfloat16)

    def tap_block(first_row, rows, positions, weights):
        row_id = lax.broadcasted_iota(jnp.int32, (rows, chunk), 0) + first_row
        value = jnp.where(row_id == positions[0], weights[0], 0.0)
        for tap in range(1, TAPS):
            value = jnp.where(row_id == positions[tap], weights[tap], value)
        return value

    def one_chunk(step, carry):
        cols = pl.ds(pl.multiple_of(step * chunk, chunk), chunk)
        weight = charge_ref[:, cols] * mask_ref[:, cols].astype(jnp.float32)
        base = [idx_ref[d:d + 1, cols] for d in range(3)]
        taps = [[w_ref[d, s:s + 1, cols] for s in range(TAPS)] for d in range(3)]
        taps[0] = [tap * weight for tap in taps[0]]
        pos_x = [base[0] + s for s in range(TAPS)]
        pos_x = [jnp.where(pos >= grid_n, pos - grid_n, pos) for pos in pos_x]
        pos_y = [base[1] + s for s in range(TAPS)]
        pos_z = [base[2] + s for s in range(TAPS)]
        for row in range(0, top_a, 16):
            high, low = split_value(tap_block(row, 16, pos_x, taps[0]))
            a_hi[row:row + 16, :] = high
            a_lo[row:row + 16, :] = low
        for row in range(0, y_ref.shape[0], 8):
            y_ref[row:row + 8, :] = tap_block(row, 8, pos_y, taps[1])
        for row in range(0, 64, 8):
            z_ref[row:row + 8, :] = tap_block(row, 8, pos_z, taps[2])
        for first in range(0, rows_y, group):
            for y in range(first, first + group):
                line_y = y_ref[y:y + 1, :]
                for row in range(0, 64, 16):
                    high, low = split_value(line_y * z_ref[row:row + 16, :])
                    b_hi[y * 64 + row:y * 64 + row + 16, :] = high
                    b_lo[y * 64 + row:y * 64 + row + 16, :] = low
            block = slice(first * 64, (first + group) * 64)
            out_ref[block, :] += (dot_nt(b_hi[block, :], a_hi[...]) + dot_nt(b_lo[block, :], a_hi[...])
                                  + dot_nt(b_hi[block, :], a_lo[...]))
        return carry

    lax.fori_loop(0, slots // chunk, one_chunk, 0)


def modes_kernel(sizes, q_ref, bc_ref, fx_hi, fx_lo, fy_hi, fy_lo, wz_hi, wz_lo, flip_ref, ek_ref, energy_ref,
                 send_x, recv_x, send_y, recv_y, send_m, recv_m, send_r, recv_r, part, sums_y, part_z, sums_z,
                 sem_sx, sem_rx, sem_sy, sem_ry, sem_sm, sem_rm, sem_row, sem_ey, sem_ez):
    grid_n, y_devs, z_devs, len_x, len_z, planes, rows_k, chunks = sizes
    me_y = lax.axis_index('ydom')
    me_z = lax.axis_index('zdom')
    away_y = y_devs - 1 - me_y
    away_z = z_devs - 1 - me_z
    row_z = lax.rem(z_devs - me_z, z_devs)
    mirror = {'ydom': away_y, 'zdom': away_z}
    mirror_row = {'ydom': away_y, 'zdom': row_z}
    ring_y = [lax.rem(me_y + k, y_devs) for k in range(y_devs)]
    ring_z = [lax.rem(me_z + k, z_devs) for k in range(z_devs)]

    barrier = pltpu.get_barrier_semaphore()
    peers = [{'ydom': dest} for dest in ring_y[1:]] + [{'zdom': dest} for dest in ring_z[1:]] + [mirror, mirror_row]
    for peer in peers:
        pl.semaphore_signal(barrier, inc=1, device_id=peer, device_id_type=MESH)

    def remote(src, dst, send_sem, recv_sem, peer):
        return pltpu.make_async_remote_copy(src_ref=src, dst_ref=dst, send_sem=send_sem, recv_sem=recv_sem,
                                            device_id=peer, device_id_type=MESH)

    lane = lax.broadcasted_iota(jnp.int32, (1, LANES), 1)
    is_low = lane < 64
    all_kx = y_devs * planes

    for quad in range(q_ref.shape[0] // 256):
        high, low = split_value(q_ref[quad * 256:(quad + 1) * 256, :])
        block = dot_nt(fx_hi[...], high) + dot_nt(fx_lo[...], high) + dot_nt(fx_hi[...], low)
        for half in range(2):
            real = block[:all_kx, half * LANES:(half + 1) * LANES]
            imag = block[all_kx:, half * LANES:(half + 1) * LANES]
            y = 4 * quad + 2 * half
            send_x[pl.ds(y, all_kx, stride=32), :] = jnp.where(is_low, real, pltpu.roll(imag, 64, 1))
            send_x[pl.ds(y + 1, all_kx, stride=32), :] = jnp.where(is_low, pltpu.roll(real, 64, 1), imag)

    pl.semaphore_wait(barrier, len(peers))

    copies_x = []
    for c, (first, last) in enumerate(chunks):
        rows = (last - first) * 32
        group = []
        for k in range(1, y_devs):
            start = pl.multiple_of(ring_y[k] * (planes * 32) + first * 32, 32)
            copy = remote(send_x.at[pl.ds(start, rows), :], recv_x.at[me_y, pl.ds(first * 32, rows), :],
                          sem_sx.at[c, k], sem_rx.at[c, k], {'ydom': ring_y[k]})
            copy.start()
            group.append(copy)
        copies_x.append(group)
    recv_x[me_y] = send_x[pl.ds(pl.multiple_of(me_y * (planes * 32), 32), planes * 32), :]

    sign = jnp.where(is_low, 1.0, -1.0)
    half_ky = z_devs * rows_k
    copies_y = []
    for c, (first, last) in enumerate(chunks):
        for copy in copies_x[c]:
            copy.wait_recv()
        for p in range(first, last, 2):
            cols = []
            for kx in (p, p + 1):
                cols.append(jnp.concatenate([recv_x[s, kx * 32:(kx + 1) * 32, :] for s in range(y_devs)], axis=0))
            high, low = split_value(jnp.concatenate(cols, axis=1))
            block = dot_f32(fy_hi[...], high) + dot_f32(fy_lo[...], high) + dot_f32(fy_hi[...], low)
            for n, kx in enumerate((p, p + 1)):
                cos_part = block[:half_ky, n * LANES:(n + 1) * LANES]
                sin_part = block[half_ky:, n * LANES:(n + 1) * LANES]
                value = cos_part + pltpu.roll(sin_part, 64, 1) * sign
                for dest in range(z_devs):
                    send_y[dest, kx * rows_k:(kx + 1) * rows_k, :] = value[dest * rows_k:(dest + 1) * rows_k, :]
        rows = slice(first * rows_k, last * rows_k)
        group = []
        for k in range(1, z_devs):
            copy = remote(send_y.at[ring_z[k], rows, :], recv_y.at[me_z, rows, :],
                          sem_sy.at[c, k], sem_ry.at[c, k], {'zdom': ring_z[k]})
            copy.start()
            group.append(copy)
        copies_y.append(group)
        recv_y[me_z, rows, :] = send_y[me_z, rows, :]

    width = wz_hi.shape[1] // 4
    total = jnp.zeros((len_z, grid_n), jnp.float32)
    send_r[...] = jnp.zeros_like(send_r)
    copies_m = []
    for c, (first, last) in enumerate(chunks):
        for copy in copies_y[c]:
            copy.wait_recv()
        rows = slice(first * rows_k, last * rows_k)
        high, low = split_value(jnp.concatenate([recv_y[s, rows, :] for s in range(z_devs)], axis=1))
        block = dot_f32(high, wz_hi[...]) + dot_f32(low, wz_hi[...]) + dot_f32(high, wz_lo[...])
        parts = [block[:, n * width:(n + 1) * width] for n in range(4)]
        power = parts[0] * parts[0] + parts[1] * parts[1]
        power_rev = parts[2] * parts[2] + parts[3] * parts[3]
        for kx in range(first, last):
            at = (kx - first) * rows_k
            value = 0.5 * bc_ref[kx] * power[at:at + len_z, :grid_n]
            ek_ref[kx] = value
            total = total + value
            if kx >= 1:
                high, low = split_value(power_rev[at:at + rows_k, :])
                flipped = dot_f32(flip_ref[...], high) + dot_f32(flip_ref[...], low)
                send_m[kx] = flipped
                send_r[kx:kx + 1, :] = flipped[0:1, :]
        low_kx = max(first, 1)
        copy = remote(send_m.at[low_kx:last], recv_m.at[low_kx:last], sem_sm.at[c], sem_rm.at[c], mirror)
        copy.start()
        copies_m.append(copy)
    copy_row = remote(send_r, recv_r, sem_row.at[0], sem_row.at[1], mirror_row)
    copy_row.start()

    copy_row.wait_recv()
    is_first = lax.broadcasted_iota(jnp.int32, (len_z, grid_n), 0) == 0
    for c, (first, last) in enumerate(chunks):
        copies_m[c].wait_recv()
        for kx in range(max(first, 1), last):
            plane = len_x - kx
            power = jnp.where(is_first, recv_r[kx:kx + 1, :grid_n], recv_m[kx, :len_z, :grid_n])
            value = 0.5 * bc_ref[plane] * power
            ek_ref[plane] = value
            total = total + value

    def spread_sum(value, out, sums, send_sems, axis, ring, me):
        out[...] = jnp.zeros_like(out) + value
        copies = []
        for k in range(1, len(ring)):
            copy = remote(out, sums.at[me], send_sems.at[0, k], send_sems.at[1, k], {axis: ring[k]})
            copy.start()
            copies.append(copy)
        sums[me] = jnp.zeros(out.shape, jnp.float32) + value
        for copy in copies:
            copy.wait_recv()
        result = sums[0]
        for s in range(1, len(ring)):
            result = result + sums[s]
        return result, copies

    local = jnp.sum(total, keepdims=True)
    over_z, copies_ez = spread_sum(local, part, sums_z, sem_ez, 'zdom', ring_z, me_z)
    over_all, copies_ey = spread_sum(over_z, part_z, sums_y, sem_ey, 'ydom', ring_y, me_y)
    energy_ref[...] = over_all / (grid_n * grid_n * grid_n)

    for copy in [x for g in copies_x for x in g] + [x for g in copies_y for x in g] + copies_m + [copy_row]:
        copy.wait_send()
    for copy in copies_ez + copies_ey:
        copy.wait_send()


def transforms(grid_n, y_devs, z_devs, len_x, len_y, len_z, planes, rows_k):
    unit = 2.0 * math.pi / grid_n

    def angle(freq, pos):
        return ((freq[:, None] * pos[None, :]) % grid_n) * unit

    freq = (np.arange(y_devs)[:, None] * len_x + np.arange(planes)[None, :]).reshape(-1)
    phase = angle(freq, np.arange(grid_n))
    mat_x = np.zeros((2 * y_devs * planes, 256))
    mat_x[:, :grid_n] = np.concatenate([np.cos(phase), -np.sin(phase)])
    pos = (np.arange(y_devs)[:, None] * len_y + np.arange(32)[None, :]).reshape(-1)
    used = np.tile(np.arange(32) < len_y + TAPS - 1, y_devs)
    ky = (np.arange(z_devs)[:, None] * len_z + np.arange(rows_k)[None, :]).reshape(-1)
    keep = np.tile(np.arange(rows_k) < len_z, z_devs)
    phase = angle(ky, pos)
    mask = keep[:, None] * used[None, :]
    mat_y = np.concatenate([np.cos(phase) * mask, np.sin(phase) * mask])
    pos = np.arange(64)
    used = pos < len_z + TAPS - 1
    width = round_up(grid_n, LANES)
    mat_z = np.zeros((z_devs, 2, 64, 4, width))
    for dev in range(z_devs):
        phase = angle(dev * len_z + pos, np.arange(grid_n))
        cos_part = np.cos(phase) * used[:, None]
        sin_part = np.sin(phase) * used[:, None]
        mat_z[dev, 0, :, 0, :grid_n] = cos_part
        mat_z[dev, 1, :, 0, :grid_n] = sin_part
        mat_z[dev, 0, :, 1, :grid_n] = -sin_part
        mat_z[dev, 1, :, 1, :grid_n] = cos_part
        mat_z[dev, 0, :, 2, :grid_n] = cos_part
        mat_z[dev, 1, :, 2, :grid_n] = -sin_part
        mat_z[dev, 0, :, 3, :grid_n] = sin_part
        mat_z[dev, 1, :, 3, :grid_n] = cos_part
    mat_z = mat_z.reshape(z_devs * 128, 4 * width)
    flip = np.zeros((rows_k, rows_k))
    flip[0, 0] = 1.0
    flip[np.arange(1, len_z), len_z - np.arange(1, len_z)] = 1.0
    return (*split_const(mat_x), *split_const(mat_y), *split_const(mat_z), flip.astype(jnp.bfloat16))


def solution(mesh):
    y_devs = mesh.shape['ydom']
    z_devs = mesh.shape['zdom']
    slot_spec = P(('sys', 'ydom', 'zdom'))
    mode_spec = P(('sys', 'ydom'), 'zdom', None)

    def local_energy(charge, real_mask, grid_idx, spline_w, influence):
        len_x, len_k, grid_n = influence.shape
        len_y = grid_n // y_devs
        len_z = grid_n // z_devs
        slots = charge.shape[0]
        chunk = min(1024, slots)
        rows_y = len_y + TAPS - 1
        group = 10
        width = round_up(grid_n, LANES)
        vmem = pl.BlockSpec(memory_space=pltpu.VMEM)

        spread = pl.pallas_call(
            functools.partial(spread_kernel, grid_n, rows_y, chunk, group),
            name='spread',
            out_shape=jax.ShapeDtypeStruct((32 * 64, width), jnp.float32),
            in_specs=[vmem] * 4,
            out_specs=vmem,
            scratch_shapes=[
                pltpu.VMEM((width, chunk), jnp.bfloat16),
                pltpu.VMEM((width, chunk), jnp.bfloat16),
                pltpu.VMEM((rows_y * 64, chunk), jnp.bfloat16),
                pltpu.VMEM((rows_y * 64, chunk), jnp.bfloat16),
                pltpu.VMEM((32, chunk), jnp.float32),
                pltpu.VMEM((64, chunk), jnp.float32),
            ],
            compiler_params=pltpu.CompilerParams(vmem_limit_bytes=40 * 2**20),
        )
        grid_q = spread(charge.reshape(1, slots), real_mask.reshape(1, slots), grid_idx.T,
                        jnp.transpose(spline_w, (1, 2, 0)))

        planes = (len_x + 1) // 2
        rows_k = round_up(len_k, 8)
        chunks = tuple((p, min(p + 4, planes)) for p in range(0, planes, 4))
        sizes = (grid_n, y_devs, z_devs, len_x, len_z, planes, rows_k, chunks)
        mats = transforms(grid_n, y_devs, z_devs, len_x, len_y, len_z, planes, rows_k)
        f32 = jnp.float32
        n = len(chunks)
        dma = pltpu.SemaphoreType.DMA
        modes = pl.pallas_call(
            functools.partial(modes_kernel, sizes),
            name='modes',
            out_shape=(jax.ShapeDtypeStruct(influence.shape, f32), jax.ShapeDtypeStruct((8, LANES), f32)),
            in_specs=[vmem] * (2 + len(mats)),
            out_specs=(vmem, vmem),
            scratch_shapes=[
                pltpu.VMEM((y_devs * planes * 32, LANES), f32),
                pltpu.VMEM((y_devs, planes * 32, LANES), f32),
                pltpu.VMEM((z_devs, planes * rows_k, LANES), f32),
                pltpu.VMEM((z_devs, planes * rows_k, LANES), f32),
                pltpu.VMEM((planes, rows_k, width), f32),
                pltpu.VMEM((planes, rows_k, width), f32),
                pltpu.VMEM((round_up(planes, 8), width), f32),
                pltpu.VMEM((round_up(planes, 8), width), f32),
                pltpu.VMEM((8, LANES), f32),
                pltpu.VMEM((y_devs, 8, LANES), f32),
                pltpu.VMEM((8, LANES), f32),
                pltpu.VMEM((z_devs, 8, LANES), f32),
                dma((n, y_devs)), dma((n, y_devs)), dma((n, z_devs)), dma((n, z_devs)),
                dma((n,)), dma((n,)), dma((2,)), dma((2, y_devs)), dma((2, z_devs)),
            ],
            compiler_params=pltpu.CompilerParams(collective_id=0, has_side_effects=True,
                                                 vmem_limit_bytes=56 * 2**20),
        )
        mode_energy, energy = modes(grid_q, influence, *mats)
        return mode_energy, energy[0, :1]

    return jax.shard_map(local_energy, mesh=mesh, in_specs=(slot_spec, slot_spec, P(('sys', 'ydom', 'zdom'), None), P(('sys', 'ydom', 'zdom'), None, None), mode_spec), out_specs=(mode_spec, P('sys')), check_vma=False)
```

```python
import functools
import math

import jax
import jax.numpy as jnp
import numpy as np
from jax import lax
from jax.experimental import pallas as pl
from jax.experimental.pallas import tpu as pltpu
from jax.sharding import PartitionSpec as P

MESH = pl.DeviceIdType.MESH
TAPS = 4
LANES = 128
NT_DIMS = (((1,), (1,)), ((), ()))


def round_up(value, unit):
    return -(-value // unit) * unit


def split_const(matrix):
    high = matrix.astype(jnp.bfloat16)
    low = (matrix - high.astype(np.float64)).astype(jnp.bfloat16)
    return high, low


def split_value(value):
    high = value.astype(jnp.bfloat16)
    low = (value - high.astype(jnp.float32)).astype(jnp.bfloat16)
    return high, low


def dot_f32(left, right):
    return jnp.dot(left, right, preferred_element_type=jnp.float32)


def dot_nt(left, right):
    return lax.dot_general(left, right, NT_DIMS, preferred_element_type=jnp.float32)


def encode(value, code_lane):
    lane = lax.broadcasted_iota(jnp.int32, (1, value.shape[1]), 1)
    top = jnp.max(jnp.abs(value), axis=1, keepdims=True)
    code = jnp.ceil(jnp.log2(jnp.maximum(top, 1e-35)) * 64.0) + 1.0
    steps = jnp.round(value * (jnp.exp2(code * (-1.0 / 64.0)) * 32766.0))
    return jnp.where(lane == code_lane, code, steps).astype(jnp.int32).astype(jnp.int16)


def decode(packed, code_lane):
    lane = lax.broadcasted_iota(jnp.int32, (1, packed.shape[1]), 1)
    steps = packed.astype(jnp.int32).astype(jnp.float32)
    code = steps[:, code_lane:code_lane + 1]
    return jnp.where(lane == code_lane, 0.0, steps * (jnp.exp2(code * (1.0 / 64.0)) * (1.0 / 32766.0)))


CODE = 63


def energy_kernel(sizes, charge_ref, mask_ref, idx_ref, w_ref, bc_hbm, fx_hi, fx_lo, fy_hi, fy_lo, wz_hi, wz_lo, flip_hbm,
                  ek_ref, energy_ref,
                  a_hi, a_lo, b_hi0, b_lo0, b_hi1, b_lo1, y_ref, z_ref, q_ref, wide_x,
                  bc_ref, fxh, fxl, fyh, fyl, wzh, wzl, flip_ref,
                  send_x, recv_x, send_y, recv_y, send_m, recv_m, send_r, recv_r, part, sums_y, part_z, sums_z,
                  sem_in, sem_sx, sem_rx, sem_sy, sem_ry, sem_sm, sem_rm, sem_row, sem_ey, sem_ez):
    grid_n, y_devs, z_devs, len_x, len_z, planes, rows_k, chunks, groups, chunk = sizes
    me_y = lax.axis_index('ydom')
    me_z = lax.axis_index('zdom')
    away_y = y_devs - 1 - me_y
    away_z = z_devs - 1 - me_z
    row_z = lax.rem(z_devs - me_z, z_devs)
    mirror = {'ydom': away_y, 'zdom': away_z}
    mirror_row = {'ydom': away_y, 'zdom': row_z}
    ring_y = [lax.rem(me_y + k, y_devs) for k in range(y_devs)]
    ring_z = [lax.rem(me_z + k, z_devs) for k in range(z_devs)]

    barrier = pltpu.get_barrier_semaphore()
    peers = [{'ydom': dest} for dest in ring_y[1:]] + [{'zdom': dest} for dest in ring_z[1:]] + [mirror, mirror_row]
    for peer in peers:
        pl.semaphore_signal(barrier, inc=1, device_id=peer, device_id_type=MESH)

    loads = [pltpu.make_async_copy(src, dst, sem_in.at[n]) for n, (src, dst) in enumerate(
        [(fx_hi, fxh), (fx_lo, fxl), (fy_hi, fyh), (fy_lo, fyl), (wz_hi, wzh), (wz_lo, wzl), (flip_hbm, flip_ref),
         (bc_hbm, bc_ref)])]
    for load in loads:
        load.start()

    def remote(src, dst, send_sem, recv_sem, peer):
        return pltpu.make_async_remote_copy(src_ref=src, dst_ref=dst, send_sem=send_sem, recv_sem=recv_sem,
                                            device_id=peer, device_id_type=MESH)

    lane = lax.broadcasted_iota(jnp.int32, (1, LANES), 1)
    is_low = lane < 64
    all_kx = y_devs * planes
    per_dest = planes * 8

    slots = charge_ref.shape[1]
    n_chunks = slots // chunk
    rows_a = a_hi.shape[1]
    top_a = round_up(grid_n, 16)
    for c in range(n_chunks):
        for ref in (a_hi, a_lo):
            ref[c, top_a:, :] = jnp.zeros((rows_a - top_a, chunk), jnp.bfloat16)
    rows_y = y_ref.shape[1]

    def tap_block(first_row, rows, positions, weights):
        row_id = lax.broadcasted_iota(jnp.int32, (rows, chunk), 0) + first_row
        value = jnp.where(row_id == positions[0], weights[0], 0.0)
        for tap in range(1, TAPS):
            value = jnp.where(row_id == positions[tap], weights[tap], value)
        return value

    def make_lines(c):
        cols = pl.ds(pl.multiple_of(c * chunk, chunk), chunk)
        weight = charge_ref[:, cols] * mask_ref[:, cols].astype(jnp.float32)
        base = [idx_ref[d:d + 1, cols] for d in range(3)]
        taps = [[w_ref[d, s:s + 1, cols] for s in range(TAPS)] for d in range(3)]
        taps[0] = [tap * weight for tap in taps[0]]
        pos_x = [base[0] + s for s in range(TAPS)]
        pos_x = [jnp.where(pos >= grid_n, pos - grid_n, pos) for pos in pos_x]
        pos_y = [base[1] + s for s in range(TAPS)]
        pos_z = [base[2] + s for s in range(TAPS)]
        for row in range(0, rows_y, 8):
            y_ref[c, row:row + 8, :] = tap_block(row, 8, pos_y, taps[1])
        for row in range(0, 64, 8):
            z_ref[c, row:row + 8, :] = tap_block(row, 8, pos_z, taps[2])
        for row in range(0, top_a, 16):
            high, low = split_value(tap_block(row, 16, pos_x, taps[0]))
            a_hi[c, row:row + 16, :] = high
            a_lo[c, row:row + 16, :] = low

    def make_b(g, c, high_ref, low_ref):
        for y in range(8):
            line_y = y_ref[c, pl.ds(g * 8 + y, 1), :]
            for row in range(0, 64, 16):
                high, low = split_value(line_y * z_ref[c, row:row + 16, :])
                high_ref[y * 64 + row:y * 64 + row + 16, :] = high
                low_ref[y * 64 + row:y * 64 + row + 16, :] = low

    make_lines(0)
    make_b(0, 0, b_hi0, b_lo0)
    copies_x = []
    for g, in_group in enumerate(groups):
        used = slice(0, in_group * 64)
        q_ref[...] = jnp.zeros_like(q_ref)

        def add_chunk(c, high_ref, low_ref):
            high, low = a_hi[c], a_lo[c]
            q_ref[used, :] += (dot_nt(high_ref[used, :], high) + dot_nt(low_ref[used, :], high)
                               + dot_nt(high_ref[used, :], low))

        def pair(step, carry):
            after = 2 * step + 2
            wrap = after // n_chunks
            after_c = after - wrap * n_chunks
            if g == 0:
                make_lines(2 * step + 1)
            make_b(g, 2 * step + 1, b_hi1, b_lo1)
            add_chunk(2 * step, b_hi0, b_lo0)
            if g == 0:
                make_lines(after_c)
            make_b(g + wrap, after_c, b_hi0, b_lo0)
            add_chunk(2 * step + 1, b_hi1, b_lo1)
            return carry

        lax.fori_loop(0, n_chunks // 2, pair, 0)

        if g == 0:
            loads[0].wait()
            loads[1].wait()
        for quad in range(2):
            high, low = split_value(q_ref[quad * 256:(quad + 1) * 256, :])
            block = dot_nt(fxh[...], high) + dot_nt(fxl[...], high) + dot_nt(fxh[...], low)
            for half in range(2):
                real = block[:all_kx, half * LANES:(half + 1) * LANES]
                imag = block[all_kx:, half * LANES:(half + 1) * LANES]
                y = 4 * quad + 2 * half
                wide_x[pl.ds(y, all_kx, stride=8), :] = jnp.where(is_low, real, pltpu.roll(imag, 64, 1))
                wide_x[pl.ds(y + 1, all_kx, stride=8), :] = jnp.where(is_low, pltpu.roll(real, 64, 1), imag)

        def pack_rows(step, carry, g=g):
            rows = pl.ds(pl.multiple_of(step * per_dest, 16), per_dest)
            send_x[g, rows, :] = encode(wide_x[rows, :], CODE)
            return carry

        lax.fori_loop(0, y_devs, pack_rows, 0)
        if g == 0:
            pl.semaphore_wait(barrier, len(peers))
        for k in range(1, y_devs):
            start = pl.multiple_of(ring_y[k] * per_dest, 16)
            copy = remote(send_x.at[g, pl.ds(start, per_dest), :], recv_x.at[g, me_y],
                          sem_sx.at[g, k], sem_rx.at[g, k], {'ydom': ring_y[k]})
            copy.start()
            copies_x.append(copy)
        recv_x[g, me_y] = send_x[g, pl.ds(pl.multiple_of(me_y * per_dest, 16), per_dest), :]

    for load in loads[2:]:
        load.wait()
    for copy in copies_x:
        copy.wait_recv()

    sign = jnp.where(is_low, 1.0, -1.0)
    half_ky = z_devs * rows_k
    copies_y = []
    for c, (first, last) in enumerate(chunks):
        for p in range(first, last, 2):
            cols = [[], []]
            for g in range(len(groups)):
                for s in range(y_devs):
                    both = decode(recv_x[g, s, p * 8:(p + 2) * 8, :], CODE)
                    cols[0].append(both[:8])
                    cols[1].append(both[8:])
            wide = jnp.concatenate([jnp.concatenate(col, axis=0) for col in cols], axis=1)
            high, low = split_value(wide)
            block = dot_f32(fyh[...], high) + dot_f32(fyl[...], high) + dot_f32(fyh[...], low)
            values = []
            for n in range(2):
                cos_part = block[:half_ky, n * LANES:(n + 1) * LANES]
                sin_part = block[half_ky:, n * LANES:(n + 1) * LANES]
                values.append(cos_part + pltpu.roll(sin_part, 64, 1) * sign)
            for dest in range(z_devs):
                rows = slice(dest * rows_k, (dest + 1) * rows_k)
                both = jnp.concatenate([values[0][rows], values[1][rows]], axis=0)
                send_y[dest, p * rows_k:(p + 2) * rows_k, :] = encode(both, CODE)
        rows = slice(first * rows_k, last * rows_k)
        group = []
        for k in range(1, z_devs):
            copy = remote(send_y.at[ring_z[k], rows, :], recv_y.at[me_z, rows, :],
                          sem_sy.at[c, k], sem_ry.at[c, k], {'zdom': ring_z[k]})
            copy.start()
            group.append(copy)
        copies_y.append(group)
        recv_y[me_z, rows, :] = send_y[me_z, rows, :]

    width = wzh.shape[1] // 2
    total = jnp.zeros((len_z, grid_n), jnp.float32)
    send_r[...] = jnp.zeros_like(send_r)
    copies_m = []
    for c, (first, last) in enumerate(chunks):
        for copy in copies_y[c]:
            copy.wait_recv()
        rows = slice(first * rows_k, last * rows_k)
        high, low = split_value(jnp.concatenate([decode(recv_y[s, rows, :], CODE) for s in range(z_devs)], axis=1))
        is_real = jnp.concatenate([is_low] * z_devs, axis=1)
        nil = jnp.zeros_like(high)
        from_real, from_imag = [
            dot_f32(h, wzh[...]) + dot_f32(l, wzh[...]) + dot_f32(h, wzl[...])
            for h, l in ((jnp.where(is_real, high, nil), jnp.where(is_real, low, nil)),
                         (jnp.where(is_real, nil, high), jnp.where(is_real, nil, low)))]
        both_signs = [from_real + from_imag, from_real - from_imag]
        power, power_rev = [v[:, :width] * v[:, :width] + v[:, width:] * v[:, width:] for v in both_signs]
        for p in range(first, last, 2):
            both = []
            for kx in (p, p + 1):
                at = (kx - first) * rows_k
                value = 0.5 * bc_ref[kx] * power[at:at + len_z, :grid_n]
                ek_ref[kx] = value
                total = total + value
                high, low = split_value(power_rev[at:at + rows_k, :])
                flipped = dot_f32(flip_ref[...], high) + dot_f32(flip_ref[...], low)
                send_r[kx:kx + 1, :] = flipped[0:1, :]
                both.append(flipped)
            send_m[p * rows_k:(p + 2) * rows_k, :] = encode(jnp.concatenate(both, axis=0), width - 1)
        copy = remote(send_m.at[rows, :], recv_m.at[rows, :], sem_sm.at[c], sem_rm.at[c], mirror)
        copy.start()
        copies_m.append(copy)
    copy_row = remote(send_r, recv_r, sem_row.at[0], sem_row.at[1], mirror_row)
    copy_row.start()

    copy_row.wait_recv()
    is_first = lax.broadcasted_iota(jnp.int32, (len_z, grid_n), 0) == 0
    for c, (first, last) in enumerate(chunks):
        copies_m[c].wait_recv()
        for p in range(first, last, 2):
            both = decode(recv_m[p * rows_k:(p + 2) * rows_k, :], width - 1)
            for kx in (p, p + 1):
                if kx >= 1:
                    plane = len_x - kx
                    at = (kx - p) * rows_k
                    power = jnp.where(is_first, recv_r[kx:kx + 1, :grid_n], both[at:at + len_z, :grid_n])
                    value = 0.5 * bc_ref[plane] * power
                    ek_ref[plane] = value
                    total = total + value

    def spread_sum(value, out, sums, sems, axis, ring, me):
        out[...] = jnp.zeros_like(out) + value
        copies = []
        for k in range(1, len(ring)):
            copy = remote(out, sums.at[me], sems.at[0, k], sems.at[1, k], {axis: ring[k]})
            copy.start()
            copies.append(copy)
        sums[me] = jnp.zeros(out.shape, jnp.float32) + value
        for copy in copies:
            copy.wait_recv()
        result = sums[0]
        for s in range(1, len(ring)):
            result = result + sums[s]
        return result, copies

    local = jnp.sum(total, keepdims=True)
    over_z, copies_ez = spread_sum(local, part, sums_z, sem_ez, 'zdom', ring_z, me_z)
    over_all, copies_ey = spread_sum(over_z, part_z, sums_y, sem_ey, 'ydom', ring_y, me_y)
    energy_ref[0] = over_all[0, 0] / (grid_n * grid_n * grid_n)

    for copy in copies_x + [x for g in copies_y for x in g] + copies_m + [copy_row] + copies_ez + copies_ey:
        copy.wait_send()


def transforms(grid_n, y_devs, z_devs, len_x, len_y, len_z, planes, rows_k):
    unit = 2.0 * math.pi / grid_n

    def angle(freq, pos):
        return ((freq[:, None] * pos[None, :]) % grid_n) * unit

    freq = (np.arange(y_devs)[:, None] * len_x + np.arange(planes)[None, :]).reshape(-1)
    phase = angle(freq, np.arange(grid_n))
    mat_x = np.zeros((2 * y_devs * planes, 256))
    mat_x[:, :grid_n] = np.concatenate([np.cos(phase), -np.sin(phase)])
    local_y = np.broadcast_to(np.arange(32).reshape(4, 1, 8), (4, y_devs, 8)).reshape(-1)
    pos = np.broadcast_to(np.arange(y_devs).reshape(1, y_devs, 1) * len_y, (4, y_devs, 8)).reshape(-1) + local_y
    used = local_y < len_y + TAPS - 1
    ky = (np.arange(z_devs)[:, None] * len_z + np.arange(rows_k)[None, :]).reshape(-1)
    keep = np.tile(np.arange(rows_k) < len_z, z_devs)
    phase = angle(ky, pos)
    mask = keep[:, None] * used[None, :]
    mat_y = np.concatenate([np.cos(phase) * mask, np.sin(phase) * mask])
    pos = np.arange(64)
    used = pos < len_z + TAPS - 1
    width = round_up(grid_n, LANES)
    mat_z = np.zeros((z_devs, 2, 64, 2, width))
    for dev in range(z_devs):
        phase = angle(dev * len_z + pos, np.arange(grid_n))
        cos_part = np.cos(phase) * used[:, None]
        sin_part = np.sin(phase) * used[:, None]
        mat_z[dev, 0, :, 0, :grid_n] = cos_part
        mat_z[dev, 1, :, 0, :grid_n] = sin_part
        mat_z[dev, 0, :, 1, :grid_n] = -sin_part
        mat_z[dev, 1, :, 1, :grid_n] = cos_part
    mat_z = mat_z.reshape(z_devs * 128, 2 * width)
    flip = np.zeros((rows_k, rows_k))
    flip[0, 0] = 1.0
    flip[np.arange(1, len_z), len_z - np.arange(1, len_z)] = 1.0
    return (*split_const(mat_x), *split_const(mat_y), *split_const(mat_z), flip.astype(jnp.bfloat16))


def solution(mesh):
    y_devs = mesh.shape['ydom']
    z_devs = mesh.shape['zdom']
    slot_spec = P(('sys', 'ydom', 'zdom'))
    mode_spec = P(('sys', 'ydom'), 'zdom', None)

    def local_energy(charge, real_mask, grid_idx, spline_w, influence):
        len_x, len_k, grid_n = influence.shape
        len_y = grid_n // y_devs
        len_z = grid_n // z_devs
        slots = charge.shape[0]
        chunk = 1024
        rows_y = len_y + TAPS - 1
        groups = tuple(min(8, rows_y - y) for y in range(0, rows_y, 8))
        width = round_up(grid_n, LANES)
        planes = (len_x + 1) // 2
        rows_k = round_up(len_k, 8)
        chunks = tuple((p, min(p + 4, planes)) for p in range(0, planes, 4))
        sizes = (grid_n, y_devs, z_devs, len_x, len_z, planes, rows_k, chunks, groups, chunk)
        mats = transforms(grid_n, y_devs, z_devs, len_x, len_y, len_z, planes, rows_k)
        f32, bf16, i16 = jnp.float32, jnp.bfloat16, jnp.int16
        vmem = pl.BlockSpec(memory_space=pltpu.VMEM)
        anywhere = pl.BlockSpec(memory_space=pl.ANY)
        n, n_g, n_c = len(chunks), len(groups), slots // chunk
        dma = pltpu.SemaphoreType.DMA
        mode_energy, energy = pl.pallas_call(
            functools.partial(energy_kernel, sizes),
            name='energy',
            out_shape=(jax.ShapeDtypeStruct(influence.shape, f32), jax.ShapeDtypeStruct((1,), f32)),
            in_specs=[vmem] * 4 + [anywhere] * (1 + len(mats)),
            out_specs=(vmem, pl.BlockSpec(memory_space=pltpu.SMEM)),
            scratch_shapes=[
                pltpu.VMEM((n_c, width, chunk), bf16), pltpu.VMEM((n_c, width, chunk), bf16),
                pltpu.VMEM((512, chunk), bf16), pltpu.VMEM((512, chunk), bf16),
                pltpu.VMEM((512, chunk), bf16), pltpu.VMEM((512, chunk), bf16),
                pltpu.VMEM((n_c, 8 * n_g + 8, chunk), f32), pltpu.VMEM((n_c, 64, chunk), f32),
                pltpu.VMEM((512, width), f32), pltpu.VMEM((y_devs * planes * 8, LANES), f32),
                pltpu.VMEM(influence.shape, f32), *[pltpu.VMEM(mat.shape, mat.dtype) for mat in mats],
                pltpu.VMEM((n_g, y_devs * planes * 8, LANES), i16),
                pltpu.VMEM((n_g, y_devs, planes * 8, LANES), i16),
                pltpu.VMEM((z_devs, planes * rows_k, LANES), i16),
                pltpu.VMEM((z_devs, planes * rows_k, LANES), i16),
                pltpu.VMEM((planes * rows_k, width), i16),
                pltpu.VMEM((planes * rows_k, width), i16),
                pltpu.VMEM((round_up(planes, 8), width), f32),
                pltpu.VMEM((round_up(planes, 8), width), f32),
                pltpu.VMEM((8, LANES), f32),
                pltpu.VMEM((y_devs, 8, LANES), f32),
                pltpu.VMEM((8, LANES), f32),
                pltpu.VMEM((z_devs, 8, LANES), f32),
                dma((8,)), dma((n_g, y_devs)), dma((n_g, y_devs)), dma((n, z_devs)), dma((n, z_devs)),
                dma((n,)), dma((n,)), dma((2,)), dma((2, y_devs)), dma((2, z_devs)),
            ],
            compiler_params=pltpu.CompilerParams(collective_id=0, has_side_effects=True,
                                                 vmem_limit_bytes=60 * 2**20),
        )(charge.reshape(1, slots), real_mask.reshape(1, slots), grid_idx.T, jnp.transpose(spline_w, (1, 2, 0)),
          influence, *mats)
        return mode_energy, energy

    return jax.shard_map(local_energy, mesh=mesh, in_specs=(slot_spec, slot_spec, P(('sys', 'ydom', 'zdom'), None), P(('sys', 'ydom', 'zdom'), None, None), mode_spec), out_specs=(mode_spec, P('sys')), check_vma=False)
```

```python
import functools
import math

import jax
import jax.numpy as jnp
import numpy as np
from jax import lax
from jax.experimental import pallas as pl
from jax.experimental.pallas import tpu as pltpu
from jax.sharding import PartitionSpec as P

MESH = pl.DeviceIdType.MESH
TAPS = 4
LANES = 128
NT_DIMS = (((1,), (1,)), ((), ()))


def round_up(value, unit):
    return -(-value // unit) * unit


def split_const(matrix):
    high = matrix.astype(jnp.bfloat16)
    low = (matrix - high.astype(np.float64)).astype(jnp.bfloat16)
    return high, low


def split_value(value):
    high = value.astype(jnp.bfloat16)
    low = (value - high.astype(jnp.float32)).astype(jnp.bfloat16)
    return high, low


def dot_f32(left, right):
    return jnp.dot(left, right, preferred_element_type=jnp.float32)


def dot_nt(left, right):
    return lax.dot_general(left, right, NT_DIMS, preferred_element_type=jnp.float32)


def encode(value, code_lane):
    lane = lax.broadcasted_iota(jnp.int32, (1, value.shape[1]), 1)
    top = jnp.max(jnp.abs(value), axis=1, keepdims=True)
    code = jnp.ceil(jnp.log2(jnp.maximum(top, 1e-35)) * 64.0) + 1.0
    steps = jnp.round(value * (jnp.exp2(code * (-1.0 / 64.0)) * 32766.0))
    return jnp.where(lane == code_lane, code, steps).astype(jnp.int32).astype(jnp.int16)


def decode(packed, code_lane):
    lane = lax.broadcasted_iota(jnp.int32, (1, packed.shape[1]), 1)
    steps = packed.astype(jnp.int32).astype(jnp.float32)
    code = steps[:, code_lane:code_lane + 1]
    return jnp.where(lane == code_lane, 0.0, steps * (jnp.exp2(code * (1.0 / 64.0)) * (1.0 / 32766.0)))


CODE = 15


def swap_lane_groups(arrays, unit):
    lane = lax.broadcasted_iota(jnp.int32, (1, LANES), 1)
    arrays = list(arrays)
    bit = len(arrays) // 2
    while bit:
        stays = (lane // (unit * bit)) % 2 == 0
        for low in range(len(arrays)):
            if low & bit == 0:
                a, b = arrays[low], arrays[low | bit]
                arrays[low] = jnp.where(stays, a, pltpu.roll(b, unit * bit, 1))
                arrays[low | bit] = jnp.where(stays, pltpu.roll(a, LANES - unit * bit, 1), b)
        bit //= 2
    return arrays


def energy_kernel(sizes, charge_hbm, mask_hbm, idx_hbm, w_hbm, bc_hbm, fx_hi, fx_lo, fy_hi, fy_lo, wz_hi, wz_lo, flip_hbm,
                  ek_ref, energy_ref,
                  charge_ref, mask_ref, idx_ref, w_ref, a_hi, a_lo, b_hi0, b_lo0, b_hi1, b_lo1, y_ref, z_ref, q_ref, wide_x,
                  bc_ref, fxh, fxl, fyh, fyl, wzh, wzl, flip_ref,
                  send_x, recv_x, send_y, recv_y, send_m, recv_m, send_r, recv_r, part, sums_y, part_z, sums_z,
                  sem_in, sem_sx, sem_rx, sem_sy, sem_ry, sem_sm, sem_rm, sem_row, sem_ey, sem_ez):
    grid_n, y_devs, z_devs, len_x, len_z, planes, rows_k, chunks, groups, chunk = sizes
    me_y = lax.axis_index('ydom')
    me_z = lax.axis_index('zdom')
    away_y = y_devs - 1 - me_y
    away_z = z_devs - 1 - me_z
    row_z = lax.rem(z_devs - me_z, z_devs)
    mirror = {'ydom': away_y, 'zdom': away_z}
    mirror_row = {'ydom': away_y, 'zdom': row_z}
    ring_y = [lax.rem(me_y + k, y_devs) for k in range(y_devs)]
    ring_z = [lax.rem(me_z + k, z_devs) for k in range(z_devs)]

    barrier = pltpu.get_barrier_semaphore()
    peers = [{'ydom': dest} for dest in ring_y[1:]] + [{'zdom': dest} for dest in ring_z[1:]] + [mirror, mirror_row]
    for peer in peers:
        pl.semaphore_signal(barrier, inc=1, device_id=peer, device_id_type=MESH)

    loads = [pltpu.make_async_copy(src, dst, sem_in.at[n]) for n, (src, dst) in enumerate(
        [(charge_hbm, charge_ref), (mask_hbm, mask_ref), (idx_hbm, idx_ref), (w_hbm, w_ref),
         (fx_hi, fxh), (fx_lo, fxl), (fy_hi, fyh), (fy_lo, fyl), (wz_hi, wzh), (wz_lo, wzl), (flip_hbm, flip_ref),
         (bc_hbm, bc_ref)])]
    for load in loads:
        load.start()

    def remote(src, dst, send_sem, recv_sem, peer):
        return pltpu.make_async_remote_copy(src_ref=src, dst_ref=dst, send_sem=send_sem, recv_sem=recv_sem,
                                            device_id=peer, device_id_type=MESH)

    lane = lax.broadcasted_iota(jnp.int32, (1, LANES), 1)
    is_real = (lane // 16) % 2 == 0
    per_dest = 4 * 32

    slots = charge_hbm.shape[1]
    n_chunks = slots // chunk
    rows_a = a_hi.shape[1]
    top_a = round_up(grid_n, 16)
    rows_y = b_hi0.shape[0] // 16
    for c in range(n_chunks):
        for ref in (a_hi, a_lo):
            ref[c, top_a:, :] = jnp.zeros((rows_a - top_a, chunk), jnp.bfloat16)

    def tap_block(row_id, positions, weights):
        value = jnp.where(row_id == positions[0], weights[0], 0.0)
        for tap in range(1, TAPS):
            value = jnp.where(row_id == positions[tap], weights[tap], value)
        return value

    def make_lines(c, carry):
        cols = pl.ds(pl.multiple_of(c * chunk, chunk), chunk)
        weight = charge_ref[:, cols] * mask_ref[:, cols].astype(jnp.float32)
        base = [idx_ref[d:d + 1, cols] for d in range(3)]
        taps = [[w_ref[d, s:s + 1, cols] for s in range(TAPS)] for d in range(3)]
        taps[0] = [tap * weight for tap in taps[0]]
        pos_x = [base[0] + s for s in range(TAPS)]
        pos_x = [jnp.where(pos >= grid_n, pos - grid_n, pos) for pos in pos_x]
        pos_y = [base[1] + s for s in range(TAPS)]
        pos_z = [base[2] + s for s in range(TAPS)]
        eight = lax.broadcasted_iota(jnp.int32, (8, chunk), 0)
        sixteen = lax.broadcasted_iota(jnp.int32, (16, chunk), 0)
        for row in range(0, y_ref.shape[1], 8):
            y_ref[c, row:row + 8, :] = tap_block(eight + row, pos_y, taps[1])
        for h, (first_z, n_z) in enumerate(groups):
            row_id = jnp.where(sixteen < n_z, sixteen + first_z, -1)
            z_ref[c, h * 16:(h + 1) * 16, :] = tap_block(row_id, pos_z, taps[2])
        for row in range(0, top_a, 16):
            high, low = split_value(tap_block(sixteen + row, pos_x, taps[0]))
            a_hi[c, row:row + 16, :] = high
            a_lo[c, row:row + 16, :] = low
        return carry

    def make_b(h, c, high_ref, low_ref):
        line_z = z_ref[c, pl.ds(pl.multiple_of(h * 16, 16), 16), :]
        for y in range(rows_y):
            high, low = split_value(y_ref[c, y:y + 1, :] * line_z)
            high_ref[y * 16:(y + 1) * 16, :] = high
            low_ref[y * 16:(y + 1) * 16, :] = low

    used = slice(0, rows_y * 16)

    def add_chunk(c, high_ref, low_ref):
        high, low = a_hi[c], a_lo[c]
        q_ref[used, :] += dot_nt(high_ref[...], high) + dot_nt(low_ref[...], high) + dot_nt(high_ref[...], low)

    sign_rows = z_devs * rows_k
    copies_x, copies_y = [], []

    def y_direction(h):
        for copy in copies_x[h]:
            copy.wait_recv()
        def two_rows_of_planes(p, carry):
            cols = []
            for n in range(2):
                lines = pl.ds(pl.multiple_of(p * 64 + n * 32, 32), 32)
                cols.append(jnp.concatenate([decode(recv_x[h, s, lines, :], CODE) for s in range(y_devs)], axis=0))
            high, low = split_value(jnp.concatenate(cols, axis=1))
            block = dot_f32(fyh[...], high) + dot_f32(fyl[...], high) + dot_f32(fyh[...], low)
            values = []
            for n in range(2):
                cos_part = block[:sign_rows, n * LANES:(n + 1) * LANES]
                sin_part = block[sign_rows:, n * LANES:(n + 1) * LANES]
                values.append(cos_part + jnp.where(is_real, pltpu.roll(sin_part, LANES - 16, 1),
                                                   -pltpu.roll(sin_part, 16, 1)))
            for dest in range(z_devs):
                rows = slice(dest * rows_k, (dest + 1) * rows_k)
                both = jnp.concatenate([values[0][rows], values[1][rows]], axis=0)
                send_y[dest, h, pl.ds(pl.multiple_of(p * 2 * rows_k, 16), 2 * rows_k), :] = encode(both, CODE)
            return carry

        lax.fori_loop(0, 2, two_rows_of_planes, 0)
        group = []
        for k in range(1, z_devs):
            copy = remote(send_y.at[ring_z[k], h], recv_y.at[me_z, h], sem_sy.at[h, k], sem_ry.at[h, k],
                          {'zdom': ring_z[k]})
            copy.start()
            group.append(copy)
        copies_y.append(group)
        recv_y[me_z, h] = send_y[me_z, h]

    for load in loads[:4]:
        load.wait()
    lax.fori_loop(0, n_chunks, make_lines, 0)
    make_b(0, 0, b_hi0, b_lo0)
    for h in range(len(groups)):
        q_ref[...] = jnp.zeros_like(q_ref)

        def pair(step, carry, h=h):
            after = 2 * step + 2
            wrap = after // n_chunks
            after_c = after - wrap * n_chunks
            make_b(h, 2 * step + 1, b_hi1, b_lo1)
            add_chunk(2 * step, b_hi0, b_lo0)
            make_b(h + wrap, after_c, b_hi0, b_lo0)
            add_chunk(2 * step + 1, b_hi1, b_lo1)
            return carry

        lax.fori_loop(0, n_chunks // 2, pair, 0)

        if h == 0:
            for load in loads[4:]:
                load.wait()
        for half in range(2):
            high, low = split_value(q_ref[half * 256:(half + 1) * 256, :])
            block = dot_nt(fxh[...], high) + dot_nt(fxl[...], high) + dot_nt(fxh[...], low)
            for tile in range(2):
                lanes = slice(tile * LANES, (tile + 1) * LANES)
                by_y = swap_lane_groups([block[b * 32:(b + 1) * 32, lanes] for b in range(8)], 16)
                for y in range(8):
                    wide_x[pl.ds((half * 2 + tile) * 8 + y, 4 * y_devs, stride=40), :] = by_y[y]

        def pack_rows(dest, carry, h=h):
            for tq in range(4):
                rows = pl.ds(pl.multiple_of((dest * 4 + tq) * 40, 8), 32)
                send_x[h, pl.ds(pl.multiple_of(dest * per_dest + tq * 32, 32), 32), :] = encode(wide_x[rows, :], CODE)
            return carry

        lax.fori_loop(0, y_devs, pack_rows, 0)
        if h == 0:
            pl.semaphore_wait(barrier, len(peers))
        group = []
        for k in range(1, y_devs):
            start = pl.multiple_of(ring_y[k] * per_dest, 16)
            copy = remote(send_x.at[h, pl.ds(start, per_dest), :], recv_x.at[h, me_y],
                          sem_sx.at[h, k], sem_rx.at[h, k], {'ydom': ring_y[k]})
            copy.start()
            group.append(copy)
        copies_x.append(group)
        recv_x[h, me_y] = send_x[h, pl.ds(pl.multiple_of(me_y * per_dest, 16), per_dest), :]
        if h >= 1:
            y_direction(h - 1)
    y_direction(len(groups) - 1)

    width = wzh.shape[1] // 2
    total = jnp.zeros((len_z, grid_n), jnp.float32)
    send_r[...] = jnp.zeros_like(send_r)
    copies_m = []
    for copy in [copy for group in copies_y for copy in group]:
        copy.wait_recv()
    real_wide = jnp.concatenate([is_real] * z_devs, axis=1)
    for c, (first, last) in enumerate(chunks):
        rows = slice(first * rows_k, last * rows_k)
        if c % 2 == 0:
            lines = slice(c * rows_k, (c + 2) * rows_k)
            by_plane = [swap_lane_groups([decode(recv_y[s, h, lines, :], CODE) for h in range(4)], 32)
                        for s in range(z_devs)]
        at = slice((c % 2) * rows_k, (c % 2 + 1) * rows_k)
        high, low = split_value(jnp.concatenate(
            [jnp.concatenate([by_plane[s][n][at] for s in range(z_devs)], axis=1) for n in range(last - first)], axis=0))
        nil = jnp.zeros_like(high)
        from_real, from_imag = [
            dot_f32(h, wzh[...]) + dot_f32(l, wzh[...]) + dot_f32(h, wzl[...])
            for h, l in ((jnp.where(real_wide, high, nil), jnp.where(real_wide, low, nil)),
                         (jnp.where(real_wide, nil, high), jnp.where(real_wide, nil, low)))]
        both_signs = [from_real + from_imag, from_real - from_imag]
        power, power_rev = [v[:, :width] * v[:, :width] + v[:, width:] * v[:, width:] for v in both_signs]
        for p in range(first, last, 2):
            both = []
            for kx in (p, p + 1):
                at = (kx - first) * rows_k
                value = 0.5 * bc_ref[kx] * power[at:at + len_z, :grid_n]
                ek_ref[kx] = value
                total = total + value
                high, low = split_value(power_rev[at:at + rows_k, :])
                flipped = dot_f32(flip_ref[...], high) + dot_f32(flip_ref[...], low)
                send_r[kx:kx + 1, :] = flipped[0:1, :]
                both.append(flipped)
            send_m[p * rows_k:(p + 2) * rows_k, :] = encode(jnp.concatenate(both, axis=0), width - 1)
        copy = remote(send_m.at[rows, :], recv_m.at[rows, :], sem_sm.at[c], sem_rm.at[c], mirror)
        copy.start()
        copies_m.append(copy)
    copy_row = remote(send_r, recv_r, sem_row.at[0], sem_row.at[1], mirror_row)
    copy_row.start()

    copy_row.wait_recv()
    is_first = lax.broadcasted_iota(jnp.int32, (len_z, grid_n), 0) == 0
    for c, (first, last) in enumerate(chunks):
        copies_m[c].wait_recv()
        for p in range(first, last, 2):
            both = decode(recv_m[p * rows_k:(p + 2) * rows_k, :], width - 1)
            for kx in (p, p + 1):
                if kx >= 1:
                    plane = len_x - kx
                    at = (kx - p) * rows_k
                    power = jnp.where(is_first, recv_r[kx:kx + 1, :grid_n], both[at:at + len_z, :grid_n])
                    value = 0.5 * bc_ref[plane] * power
                    ek_ref[plane] = value
                    total = total + value

    def spread_sum(value, out, sums, sems, axis, ring, me):
        out[...] = jnp.zeros_like(out) + value
        copies = []
        for k in range(1, len(ring)):
            copy = remote(out, sums.at[me], sems.at[0, k], sems.at[1, k], {axis: ring[k]})
            copy.start()
            copies.append(copy)
        sums[me] = jnp.zeros(out.shape, jnp.float32) + value
        for copy in copies:
            copy.wait_recv()
        result = sums[0]
        for s in range(1, len(ring)):
            result = result + sums[s]
        return result, copies

    local = jnp.sum(total, keepdims=True)
    over_z, copies_ez = spread_sum(local, part, sums_z, sem_ez, 'zdom', ring_z, me_z)
    over_all, copies_ey = spread_sum(over_z, part_z, sums_y, sem_ey, 'ydom', ring_y, me_y)
    energy_ref[0] = over_all[0, 0] / (grid_n * grid_n * grid_n)

    for copy in [x for g in copies_x + copies_y for x in g] + copies_m + [copy_row] + copies_ez + copies_ey:
        copy.wait_send()


def transforms(grid_n, y_devs, z_devs, len_x, len_y, len_z, planes, rows_k, groups):
    unit = 2.0 * math.pi / grid_n

    def angle(freq, pos):
        return ((freq[:, None] * pos[None, :]) % grid_n) * unit

    plane = np.arange(4)[None, None, :] * 4 + np.arange(4)[:, None, None]
    freq = (np.arange(y_devs)[None, :, None] * len_x + plane).reshape(-1)
    keep = np.broadcast_to(plane < planes, (4, y_devs, 4)).reshape(-1)
    phase = angle(freq, np.arange(grid_n))
    mat_x = np.zeros((4, 2, y_devs * 4, round_up(grid_n, LANES)))
    mat_x[:, 0, :, :grid_n] = (np.cos(phase) * keep[:, None]).reshape(4, y_devs * 4, grid_n)
    mat_x[:, 1, :, :grid_n] = (-np.sin(phase) * keep[:, None]).reshape(4, y_devs * 4, grid_n)
    mat_x = mat_x.reshape(8 * y_devs * 4, -1)
    pos = (np.arange(y_devs)[:, None] * len_y + np.arange(32)[None, :]).reshape(-1)
    used = np.tile(np.arange(32) < len_y + TAPS - 1, y_devs)
    ky = (np.arange(z_devs)[:, None] * len_z + np.arange(rows_k)[None, :]).reshape(-1)
    keep = np.tile(np.arange(rows_k) < len_z, z_devs)
    phase = angle(ky, pos)
    mask = keep[:, None] * used[None, :]
    mat_y = np.concatenate([np.cos(phase) * mask, np.sin(phase) * mask])
    width = round_up(grid_n, LANES)
    mat_z = np.zeros((z_devs, len(groups), 2, 16, 2, width))
    for dev in range(z_devs):
        for h, (first_z, n_z) in enumerate(groups):
            phase = angle(dev * len_z + first_z + np.arange(n_z), np.arange(grid_n))
            mat_z[dev, h, 0, :n_z, 0, :grid_n] = np.cos(phase)
            mat_z[dev, h, 1, :n_z, 0, :grid_n] = np.sin(phase)
            mat_z[dev, h, 0, :n_z, 1, :grid_n] = -np.sin(phase)
            mat_z[dev, h, 1, :n_z, 1, :grid_n] = np.cos(phase)
    mat_z = mat_z.reshape(z_devs * 128, 2 * width)
    flip = np.zeros((rows_k, rows_k))
    flip[0, 0] = 1.0
    flip[np.arange(1, len_z), len_z - np.arange(1, len_z)] = 1.0
    return (*split_const(mat_x), *split_const(mat_y), *split_const(mat_z), flip.astype(jnp.bfloat16))


def solution(mesh):
    y_devs = mesh.shape['ydom']
    z_devs = mesh.shape['zdom']
    slot_spec = P(('sys', 'ydom', 'zdom'))
    mode_spec = P(('sys', 'ydom'), 'zdom', None)

    def local_energy(charge, real_mask, grid_idx, spline_w, influence):
        len_x, len_k, grid_n = influence.shape
        len_y = grid_n // y_devs
        len_z = grid_n // z_devs
        slots = charge.shape[0]
        chunk = 1024
        rows_y = len_y + TAPS - 1
        rows_z = len_z + TAPS - 1
        cuts = [-(-rows_z * h // 4) for h in range(5)]
        groups = tuple((cuts[h], cuts[h + 1] - cuts[h]) for h in range(4))
        width = round_up(grid_n, LANES)
        planes = (len_x + 1) // 2
        rows_k = round_up(len_k, 8)
        chunks = tuple((p, min(p + 4, planes)) for p in range(0, planes, 4))
        sizes = (grid_n, y_devs, z_devs, len_x, len_z, planes, rows_k, chunks, groups, chunk)
        mats = transforms(grid_n, y_devs, z_devs, len_x, len_y, len_z, planes, rows_k, groups)
        f32, bf16, i16 = jnp.float32, jnp.bfloat16, jnp.int16
        vmem = pl.BlockSpec(memory_space=pltpu.VMEM)
        hbm = pl.BlockSpec(memory_space=pltpu.HBM)
        n, n_g, n_c = len(chunks), len(groups), slots // chunk
        dma = pltpu.SemaphoreType.DMA
        mode_energy, energy = pl.pallas_call(
            functools.partial(energy_kernel, sizes),
            name='energy',
            out_shape=(jax.ShapeDtypeStruct(influence.shape, f32), jax.ShapeDtypeStruct((1,), f32)),
            in_specs=[hbm] * (5 + len(mats)),
            out_specs=(vmem, pl.BlockSpec(memory_space=pltpu.SMEM)),
            scratch_shapes=[
                pltpu.VMEM((1, slots), f32), pltpu.VMEM((1, slots), jnp.int32), pltpu.VMEM((3, slots), jnp.int32),
                pltpu.VMEM((3, TAPS, slots), f32),
                pltpu.VMEM((n_c, width, chunk), bf16), pltpu.VMEM((n_c, width, chunk), bf16),
                *[pltpu.VMEM((rows_y * 16, chunk), bf16)] * 4,
                pltpu.VMEM((n_c, 32, chunk), f32), pltpu.VMEM((n_c, 16 * n_g + 16, chunk), f32),
                pltpu.VMEM((512, width), f32), pltpu.VMEM((y_devs * 4 * 40, LANES), f32),
                pltpu.VMEM(influence.shape, f32), *[pltpu.VMEM(mat.shape, mat.dtype) for mat in mats],
                pltpu.VMEM((n_g, y_devs * 128, LANES), i16),
                pltpu.VMEM((n_g, y_devs, 128, LANES), i16),
                pltpu.VMEM((z_devs, n_g, 4 * rows_k, LANES), i16),
                pltpu.VMEM((z_devs, n_g, 4 * rows_k, LANES), i16),
                pltpu.VMEM((planes * rows_k, width), i16),
                pltpu.VMEM((planes * rows_k, width), i16),
                pltpu.VMEM((round_up(planes, 8), width), f32),
                pltpu.VMEM((round_up(planes, 8), width), f32),
                pltpu.VMEM((8, LANES), f32),
                pltpu.VMEM((y_devs, 8, LANES), f32),
                pltpu.VMEM((8, LANES), f32),
                pltpu.VMEM((z_devs, 8, LANES), f32),
                dma((12,)), dma((n_g, y_devs)), dma((n_g, y_devs)), dma((n_g, z_devs)), dma((n_g, z_devs)),
                dma((n,)), dma((n,)), dma((2,)), dma((2, y_devs)), dma((2, z_devs)),
            ],
            compiler_params=pltpu.CompilerParams(collective_id=0, has_side_effects=True,
                                                 vmem_limit_bytes=60 * 2**20),
        )(charge.reshape(1, slots), real_mask.reshape(1, slots), grid_idx.T, jnp.transpose(spline_w, (1, 2, 0)),
          influence, *mats)
        return mode_energy, energy

    return jax.shard_map(local_energy, mesh=mesh, in_specs=(slot_spec, slot_spec, P(('sys', 'ydom', 'zdom'), None), P(('sys', 'ydom', 'zdom'), None, None), mode_spec), out_specs=(mode_spec, P('sys')), check_vma=False)
```

```python
import functools
import math

import jax
import jax.numpy as jnp
import numpy as np
from jax import lax
from jax.experimental import pallas as pl
from jax.experimental.pallas import tpu as pltpu
from jax.sharding import PartitionSpec as P

MESH = pl.DeviceIdType.MESH
TAPS = 4
LANES = 128
NT_DIMS = (((1,), (1,)), ((), ()))


def round_up(value, unit):
    return -(-value // unit) * unit


def split_const(matrix):
    high = matrix.astype(jnp.bfloat16)
    low = (matrix - high.astype(np.float64)).astype(jnp.bfloat16)
    return high, low


def split_value(value):
    high = value.astype(jnp.bfloat16)
    low = (value - high.astype(jnp.float32)).astype(jnp.bfloat16)
    return high, low


def dot_f32(left, right):
    return jnp.dot(left, right, preferred_element_type=jnp.float32)


def dot_nt(left, right):
    return lax.dot_general(left, right, NT_DIMS, preferred_element_type=jnp.float32)


def encode(value, code_lane):
    lane = lax.broadcasted_iota(jnp.int32, (1, value.shape[1]), 1)
    top = jnp.max(jnp.abs(value), axis=1, keepdims=True)
    code = jnp.ceil(jnp.log2(jnp.maximum(top, 1e-35)) * 64.0) + 1.0
    steps = jnp.round(value * (jnp.exp2(code * (-1.0 / 64.0)) * 32766.0))
    return jnp.where(lane == code_lane, code, steps).astype(jnp.int32).astype(jnp.int16)


def decode(packed, code_lane):
    lane = lax.broadcasted_iota(jnp.int32, (1, packed.shape[1]), 1)
    steps = packed.astype(jnp.int32).astype(jnp.float32)
    code = steps[:, code_lane:code_lane + 1]
    return jnp.where(lane == code_lane, 0.0, steps * (jnp.exp2(code * (1.0 / 64.0)) * (1.0 / 32766.0)))


CODE = 15


def swap_lane_groups(arrays, unit):
    lane = lax.broadcasted_iota(jnp.int32, (1, LANES), 1)
    arrays = list(arrays)
    bit = len(arrays) // 2
    while bit:
        stays = (lane // (unit * bit)) % 2 == 0
        for low in range(len(arrays)):
            if low & bit == 0:
                a, b = arrays[low], arrays[low | bit]
                arrays[low] = jnp.where(stays, a, pltpu.roll(b, unit * bit, 1))
                arrays[low | bit] = jnp.where(stays, pltpu.roll(a, LANES - unit * bit, 1), b)
        bit //= 2
    return arrays


def energy_kernel(sizes, charge_hbm, mask_hbm, idx_hbm, w_hbm, bc_hbm, fx_hi, fx_lo, fy_hi, fy_lo, wz_hi, wz_lo, flip_hbm,
                  ek_ref, energy_ref,
                  charge_ref, mask_ref, idx_ref, w_ref, a_hi, a_lo, b_hi0, b_lo0, b_hi1, b_lo1, y_ref, z_ref, q_ref, wide_x,
                  bc_ref, fxh, fxl, fyh, fyl, wzh, wzl, flip_ref,
                  send_x, recv_x, send_y, recv_y, send_m, recv_m, send_r, recv_r, bc_mirror, bc_row, wide_m, part, sums_y, part_z, sums_z,
                  sem_in, sem_sx, sem_rx, sem_sy, sem_ry, sem_sm, sem_rm, sem_row, sem_ey, sem_ez, sem_bc):
    grid_n, y_devs, z_devs, len_x, len_z, planes, rows_k, chunks, groups, chunk = sizes
    me_y = lax.axis_index('ydom')
    me_z = lax.axis_index('zdom')
    away_y = y_devs - 1 - me_y
    away_z = z_devs - 1 - me_z
    row_z = lax.rem(z_devs - me_z, z_devs)
    mirror = {'ydom': away_y, 'zdom': away_z}
    mirror_row = {'ydom': away_y, 'zdom': row_z}
    ring_y = [lax.rem(me_y + k, y_devs) for k in range(y_devs)]
    ring_z = [lax.rem(me_z + k, z_devs) for k in range(z_devs)]

    barrier = pltpu.get_barrier_semaphore()
    peers = [{'ydom': dest} for dest in ring_y[1:]] + [{'zdom': dest} for dest in ring_z[1:]] + [mirror, mirror_row]
    for peer in peers:
        pl.semaphore_signal(barrier, inc=1, device_id=peer, device_id_type=MESH)

    loads = [pltpu.make_async_copy(src, dst, sem_in.at[n]) for n, (src, dst) in enumerate(
        [(charge_hbm, charge_ref), (mask_hbm, mask_ref), (idx_hbm, idx_ref), (w_hbm, w_ref),
         (fx_hi, fxh), (fx_lo, fxl), (fy_hi, fyh), (fy_lo, fyl), (wz_hi, wzh), (wz_lo, wzl), (flip_hbm, flip_ref),
         (bc_hbm, bc_ref)])]
    for load in loads:
        load.start()

    def remote(src, dst, send_sem, recv_sem, peer):
        return pltpu.make_async_remote_copy(src_ref=src, dst_ref=dst, send_sem=send_sem, recv_sem=recv_sem,
                                            device_id=peer, device_id_type=MESH)

    lane = lax.broadcasted_iota(jnp.int32, (1, LANES), 1)
    is_real = (lane // 16) % 2 == 0
    per_dest = 4 * 32

    slots = charge_hbm.shape[1]
    n_chunks = slots // chunk
    rows_a = a_hi.shape[1]
    top_a = round_up(grid_n, 16)
    rows_y = b_hi0.shape[0] // 16
    for c in range(n_chunks):
        for ref in (a_hi, a_lo):
            ref[c, top_a:, :] = jnp.zeros((rows_a - top_a, chunk), jnp.bfloat16)

    def tap_block(row_id, positions, weights):
        value = jnp.where(row_id == positions[0], weights[0], 0.0)
        for tap in range(1, TAPS):
            value = jnp.where(row_id == positions[tap], weights[tap], value)
        return value

    def make_lines(c, carry):
        cols = pl.ds(pl.multiple_of(c * chunk, chunk), chunk)
        weight = charge_ref[:, cols] * mask_ref[:, cols].astype(jnp.float32)
        base = [idx_ref[d:d + 1, cols] for d in range(3)]
        taps = [[w_ref[d, s:s + 1, cols] for s in range(TAPS)] for d in range(3)]
        taps[0] = [tap * weight for tap in taps[0]]
        pos_x = [base[0] + s for s in range(TAPS)]
        pos_x = [jnp.where(pos >= grid_n, pos - grid_n, pos) for pos in pos_x]
        pos_y = [base[1] + s for s in range(TAPS)]
        pos_z = [base[2] + s for s in range(TAPS)]
        eight = lax.broadcasted_iota(jnp.int32, (8, chunk), 0)
        sixteen = lax.broadcasted_iota(jnp.int32, (16, chunk), 0)
        for row in range(0, y_ref.shape[1], 8):
            y_ref[c, row:row + 8, :] = tap_block(eight + row, pos_y, taps[1])
        for h, (first_z, n_z) in enumerate(groups):
            row_id = jnp.where(sixteen < n_z, sixteen + first_z, -1)
            z_ref[c, h * 16:(h + 1) * 16, :] = tap_block(row_id, pos_z, taps[2])
        for row in range(0, top_a, 16):
            high, low = split_value(tap_block(sixteen + row, pos_x, taps[0]))
            a_hi[c, row:row + 16, :] = high
            a_lo[c, row:row + 16, :] = low
        return carry

    def make_b(h, c, high_ref, low_ref):
        line_z = z_ref[c, pl.ds(pl.multiple_of(h * 16, 16), 16), :]
        for y in range(rows_y):
            high, low = split_value(y_ref[c, y:y + 1, :] * line_z)
            high_ref[y * 16:(y + 1) * 16, :] = high
            low_ref[y * 16:(y + 1) * 16, :] = low

    used = slice(0, rows_y * 16)

    def add_chunk(c, high_ref, low_ref):
        high, low = a_hi[c], a_lo[c]
        q_ref[used, :] += dot_nt(high_ref[...], high) + dot_nt(low_ref[...], high) + dot_nt(high_ref[...], low)

    sign_rows = z_devs * rows_k

    def y_half(h, p):
        cols = []
        for n in range(2):
            lines = pl.ds(pl.multiple_of(p * 64 + n * 32, 32), 32)
            cols.append(jnp.concatenate([decode(recv_x[h, s, lines, :], CODE) for s in range(y_devs)], axis=0))
        high, low = split_value(jnp.concatenate(cols, axis=1))
        block = dot_f32(fyh[...], high) + dot_f32(fyl[...], high) + dot_f32(fyh[...], low)
        values = []
        for n in range(2):
            cos_part = block[:sign_rows, n * LANES:(n + 1) * LANES]
            sin_part = block[sign_rows:, n * LANES:(n + 1) * LANES]
            values.append(cos_part + jnp.where(is_real, pltpu.roll(sin_part, LANES - 16, 1),
                                               -pltpu.roll(sin_part, 16, 1)))
        for dest in range(z_devs):
            rows = slice(dest * rows_k, (dest + 1) * rows_k)
            both = jnp.concatenate([values[0][rows], values[1][rows]], axis=0)
            send_y[dest, h, pl.ds(pl.multiple_of(p * 2 * rows_k, 16), 2 * rows_k), :] = encode(both, CODE)

    def x_copy(h, p, k):
        start = pl.multiple_of(ring_y[k] * per_dest + p * 64, 64)
        return remote(send_x.at[h, pl.ds(start, 64), :], recv_x.at[h, me_y, pl.ds(pl.multiple_of(p * 64, 64), 64), :],
                      sem_sx.at[2 * h + p, k], sem_rx.at[2 * h + p, k], {'ydom': ring_y[k]})

    def y_copy(h, p, k):
        rows = pl.ds(pl.multiple_of(p * 2 * rows_k, 16), 2 * rows_k)
        return remote(send_y.at[ring_z[k], h, rows, :], recv_y.at[me_z, h, rows, :],
                      sem_sy.at[2 * h + p, k], sem_ry.at[2 * h + p, k], {'zdom': ring_z[k]})

    def y_direction(h):
        def one_half(p, carry):
            for k in range(1, y_devs):
                x_copy(h, p, k).wait_recv()
            y_half(h, p)
            for k in range(1, z_devs):
                y_copy(h, p, k).start()
            rows = pl.ds(pl.multiple_of(p * 2 * rows_k, 16), 2 * rows_k)
            recv_y[me_z, h, rows, :] = send_y[me_z, h, rows, :]
            return carry

        lax.fori_loop(0, 2, one_half, 0)

    for load in loads[:4]:
        load.wait()
    lax.fori_loop(0, n_chunks, make_lines, 0)
    pl.semaphore_wait(barrier, len(peers))
    upper = pl.ds(planes, len_x - planes)
    copies_bc = [remote(bc_hbm.at[upper], bc_mirror, sem_bc.at[0, 0], sem_bc.at[1, 0], mirror),
                 remote(bc_hbm.at[upper, pl.ds(0, 8), :], bc_row, sem_bc.at[0, 1], sem_bc.at[1, 1], mirror_row)]
    for copy in copies_bc:
        copy.start()
    make_b(0, 0, b_hi0, b_lo0)
    for h in range(len(groups)):
        q_ref[...] = jnp.zeros_like(q_ref)

        def pair(step, carry, h=h):
            after = 2 * step + 2
            wrap = after // n_chunks
            after_c = after - wrap * n_chunks
            make_b(h, 2 * step + 1, b_hi1, b_lo1)
            add_chunk(2 * step, b_hi0, b_lo0)
            make_b(h + wrap, after_c, b_hi0, b_lo0)
            add_chunk(2 * step + 1, b_hi1, b_lo1)
            return carry

        lax.fori_loop(0, n_chunks // 2, pair, 0)

        if h == 0:
            for load in loads[4:]:
                load.wait()
        for half in range(2):
            high, low = split_value(q_ref[half * 256:(half + 1) * 256, :])
            block = dot_nt(fxh[...], high) + dot_nt(fxl[...], high) + dot_nt(fxh[...], low)
            for tile in range(2):
                lanes = slice(tile * LANES, (tile + 1) * LANES)
                by_y = swap_lane_groups([block[b * 32:(b + 1) * 32, lanes] for b in range(8)], 16)
                for y in range(8):
                    wide_x[pl.ds((half * 2 + tile) * 8 + y, 4 * y_devs, stride=40), :] = by_y[y]

        def pack_rows(dest, carry, h=h):
            for tq in range(4):
                rows = pl.ds(pl.multiple_of((dest * 4 + tq) * 40, 8), 32)
                send_x[h, pl.ds(pl.multiple_of(dest * per_dest + tq * 32, 32), 32), :] = encode(wide_x[rows, :], CODE)
            return carry

        lax.fori_loop(0, y_devs, pack_rows, 0)
        for p in range(2):
            for k in range(1, y_devs):
                x_copy(h, p, k).start()
        recv_x[h, me_y] = send_x[h, pl.ds(pl.multiple_of(me_y * per_dest, 16), per_dest), :]
        if h >= 1:
            y_direction(h - 1)
    y_direction(len(groups) - 1)

    width = wzh.shape[1] // 2
    total = jnp.zeros((len_z, grid_n), jnp.float32)
    is_first = lax.broadcasted_iota(jnp.int32, (len_z, grid_n), 0) == 0
    for copy in copies_bc:
        copy.wait_recv()
    send_r[...] = jnp.zeros_like(send_r)
    wide_m[...] = jnp.zeros_like(wide_m)
    copies_m = []
    real_wide = jnp.concatenate([is_real] * z_devs, axis=1)
    for c, (first, last) in enumerate(chunks):
        rows = slice(first * rows_k, last * rows_k)
        if c % 2 == 0:
            for h in range(len(groups)):
                for k in range(1, z_devs):
                    y_copy(h, c // 2, k).wait_recv()
            lines = slice(c * rows_k, (c + 2) * rows_k)
            by_plane = [swap_lane_groups([decode(recv_y[s, h, lines, :], CODE) for h in range(4)], 32)
                        for s in range(z_devs)]
        at = slice((c % 2) * rows_k, (c % 2 + 1) * rows_k)
        high, low = split_value(jnp.concatenate(
            [jnp.concatenate([by_plane[s][n][at] for s in range(z_devs)], axis=1) for n in range(last - first)], axis=0))
        nil = jnp.zeros_like(high)
        from_real, from_imag = [
            dot_f32(h, wzh[...]) + dot_f32(l, wzh[...]) + dot_f32(h, wzl[...])
            for h, l in ((jnp.where(real_wide, high, nil), jnp.where(real_wide, low, nil)),
                         (jnp.where(real_wide, nil, high), jnp.where(real_wide, nil, low)))]
        both_signs = [from_real + from_imag, from_real - from_imag]
        power, power_rev = [v[:, :width] * v[:, :width] + v[:, width:] * v[:, width:] for v in both_signs]
        for p in range(first, last, 2):
            for kx in (p, p + 1):
                at = (kx - first) * rows_k
                value = 0.5 * bc_ref[kx] * power[at:at + len_z, :grid_n]
                ek_ref[kx] = value
                total = total + value
                high, low = split_value(power_rev[at:at + rows_k, :])
                flipped = dot_f32(flip_ref[...], high) + dot_f32(flip_ref[...], low)
                if kx >= 1:
                    plane = len_x - kx - planes
                    factor = jnp.where(is_first, bc_row[plane, 0:1, :], bc_mirror[plane])
                    value = 0.5 * factor * flipped[:len_z, :grid_n]
                    total = total + value
                    send_r[kx:kx + 1, :grid_n] = value[0:1, :]
                    wide_m[(kx - p) * rows_k:(kx - p) * rows_k + len_z, :grid_n] = value
            send_m[p * rows_k:(p + 2) * rows_k, :] = encode(wide_m[...], width - 1)
        copy = remote(send_m.at[rows, :], recv_m.at[rows, :], sem_sm.at[c], sem_rm.at[c], mirror)
        copy.start()
        copies_m.append(copy)
    copy_row = remote(send_r, recv_r, sem_row.at[0], sem_row.at[1], mirror_row)
    copy_row.start()

    def start_sum(value, out, sums, sems, axis, ring, me):
        out[...] = jnp.zeros_like(out) + value
        copies = []
        for k in range(1, len(ring)):
            copy = remote(out, sums.at[me], sems.at[0, k], sems.at[1, k], {axis: ring[k]})
            copy.start()
            copies.append(copy)
        sums[me] = jnp.zeros(out.shape, jnp.float32) + value
        return copies

    def end_sum(sums, copies):
        for copy in copies:
            copy.wait_recv()
        result = sums[0]
        for s in range(1, len(copies) + 1):
            result = result + sums[s]
        return result

    copies_ez = start_sum(jnp.sum(total, keepdims=True), part, sums_z, sem_ez, 'zdom', ring_z, me_z)
    copies_ey = start_sum(end_sum(sums_z, copies_ez), part_z, sums_y, sem_ey, 'ydom', ring_y, me_y)

    copy_row.wait_recv()
    for c, (first, last) in enumerate(chunks):
        copies_m[c].wait_recv()
        for p in range(first, last, 2):
            both = decode(recv_m[p * rows_k:(p + 2) * rows_k, :], width - 1)
            for kx in (p, p + 1):
                if kx >= 1:
                    at = (kx - p) * rows_k
                    ek_ref[len_x - kx] = jnp.where(is_first, recv_r[kx:kx + 1, :grid_n], both[at:at + len_z, :grid_n])

    energy_ref[0] = end_sum(sums_y, copies_ey)[0, 0] / (grid_n * grid_n * grid_n)

    for copy in copies_m + [copy_row] + copies_ez + copies_ey + copies_bc:
        copy.wait_send()
    for h in range(len(groups)):
        for p in range(2):
            for k in range(1, y_devs):
                x_copy(h, p, k).wait_send()
            for k in range(1, z_devs):
                y_copy(h, p, k).wait_send()


def transforms(grid_n, y_devs, z_devs, len_x, len_y, len_z, planes, rows_k, groups):
    unit = 2.0 * math.pi / grid_n

    def angle(freq, pos):
        return ((freq[:, None] * pos[None, :]) % grid_n) * unit

    plane = np.arange(4)[None, None, :] * 4 + np.arange(4)[:, None, None]
    freq = (np.arange(y_devs)[None, :, None] * len_x + plane).reshape(-1)
    keep = np.broadcast_to(plane < planes, (4, y_devs, 4)).reshape(-1)
    phase = angle(freq, np.arange(grid_n))
    mat_x = np.zeros((4, 2, y_devs * 4, round_up(grid_n, LANES)))
    mat_x[:, 0, :, :grid_n] = (np.cos(phase) * keep[:, None]).reshape(4, y_devs * 4, grid_n)
    mat_x[:, 1, :, :grid_n] = (-np.sin(phase) * keep[:, None]).reshape(4, y_devs * 4, grid_n)
    mat_x = mat_x.reshape(8 * y_devs * 4, -1)
    pos = (np.arange(y_devs)[:, None] * len_y + np.arange(32)[None, :]).reshape(-1)
    used = np.tile(np.arange(32) < len_y + TAPS - 1, y_devs)
    ky = (np.arange(z_devs)[:, None] * len_z + np.arange(rows_k)[None, :]).reshape(-1)
    keep = np.tile(np.arange(rows_k) < len_z, z_devs)
    phase = angle(ky, pos)
    mask = keep[:, None] * used[None, :]
    mat_y = np.concatenate([np.cos(phase) * mask, np.sin(phase) * mask])
    width = round_up(grid_n, LANES)
    mat_z = np.zeros((z_devs, len(groups), 2, 16, 2, width))
    for dev in range(z_devs):
        for h, (first_z, n_z) in enumerate(groups):
            phase = angle(dev * len_z + first_z + np.arange(n_z), np.arange(grid_n))
            mat_z[dev, h, 0, :n_z, 0, :grid_n] = np.cos(phase)
            mat_z[dev, h, 1, :n_z, 0, :grid_n] = np.sin(phase)
            mat_z[dev, h, 0, :n_z, 1, :grid_n] = -np.sin(phase)
            mat_z[dev, h, 1, :n_z, 1, :grid_n] = np.cos(phase)
    mat_z = mat_z.reshape(z_devs * 128, 2 * width)
    flip = np.zeros((rows_k, rows_k))
    flip[0, 0] = 1.0
    flip[np.arange(1, len_z), len_z - np.arange(1, len_z)] = 1.0
    return (*split_const(mat_x), *split_const(mat_y), *split_const(mat_z), flip.astype(jnp.bfloat16))


def solution(mesh):
    y_devs = mesh.shape['ydom']
    z_devs = mesh.shape['zdom']
    slot_spec = P(('sys', 'ydom', 'zdom'))
    mode_spec = P(('sys', 'ydom'), 'zdom', None)

    def local_energy(charge, real_mask, grid_idx, spline_w, influence):
        len_x, len_k, grid_n = influence.shape
        len_y = grid_n // y_devs
        len_z = grid_n // z_devs
        slots = charge.shape[0]
        chunk = 1024
        rows_y = len_y + TAPS - 1
        rows_z = len_z + TAPS - 1
        cuts = [-(-rows_z * h // 4) for h in range(5)]
        groups = tuple((cuts[h], cuts[h + 1] - cuts[h]) for h in range(4))
        width = round_up(grid_n, LANES)
        planes = (len_x + 1) // 2
        rows_k = round_up(len_k, 8)
        chunks = tuple((p, min(p + 4, planes)) for p in range(0, planes, 4))
        sizes = (grid_n, y_devs, z_devs, len_x, len_z, planes, rows_k, chunks, groups, chunk)
        mats = transforms(grid_n, y_devs, z_devs, len_x, len_y, len_z, planes, rows_k, groups)
        f32, bf16, i16 = jnp.float32, jnp.bfloat16, jnp.int16
        vmem = pl.BlockSpec(memory_space=pltpu.VMEM)
        hbm = pl.BlockSpec(memory_space=pltpu.HBM)
        n, n_g, n_c = len(chunks), len(groups), slots // chunk
        dma = pltpu.SemaphoreType.DMA
        mode_energy, energy = pl.pallas_call(
            functools.partial(energy_kernel, sizes),
            name='energy',
            out_shape=(jax.ShapeDtypeStruct(influence.shape, f32), jax.ShapeDtypeStruct((1,), f32)),
            in_specs=[hbm] * (5 + len(mats)),
            out_specs=(vmem, pl.BlockSpec(memory_space=pltpu.SMEM)),
            scratch_shapes=[
                pltpu.VMEM((1, slots), f32), pltpu.VMEM((1, slots), jnp.int32), pltpu.VMEM((3, slots), jnp.int32),
                pltpu.VMEM((3, TAPS, slots), f32),
                pltpu.VMEM((n_c, width, chunk), bf16), pltpu.VMEM((n_c, width, chunk), bf16),
                *[pltpu.VMEM((rows_y * 16, chunk), bf16)] * 4,
                pltpu.VMEM((n_c, 32, chunk), f32), pltpu.VMEM((n_c, 16 * n_g + 16, chunk), f32),
                pltpu.VMEM((512, width), f32), pltpu.VMEM((y_devs * 4 * 40, LANES), f32),
                pltpu.VMEM(influence.shape, f32), *[pltpu.VMEM(mat.shape, mat.dtype) for mat in mats],
                pltpu.VMEM((n_g, y_devs * 128, LANES), i16),
                pltpu.VMEM((n_g, y_devs, 128, LANES), i16),
                pltpu.VMEM((z_devs, n_g, 4 * rows_k, LANES), i16),
                pltpu.VMEM((z_devs, n_g, 4 * rows_k, LANES), i16),
                pltpu.VMEM((planes * rows_k, width), i16),
                pltpu.VMEM((planes * rows_k, width), i16),
                pltpu.VMEM((round_up(planes, 8), width), f32),
                pltpu.VMEM((round_up(planes, 8), width), f32),
                pltpu.VMEM((len_x - planes, len_k, grid_n), f32),
                pltpu.VMEM((len_x - planes, 8, grid_n), f32),
                pltpu.VMEM((2 * rows_k, width), f32),
                pltpu.VMEM((8, LANES), f32),
                pltpu.VMEM((y_devs, 8, LANES), f32),
                pltpu.VMEM((8, LANES), f32),
                pltpu.VMEM((z_devs, 8, LANES), f32),
                dma((12,)), dma((2 * n_g, y_devs)), dma((2 * n_g, y_devs)), dma((2 * n_g, z_devs)), dma((2 * n_g, z_devs)),
                dma((n,)), dma((n,)), dma((2,)), dma((2, y_devs)), dma((2, z_devs)), dma((2, 2)),
            ],
            compiler_params=pltpu.CompilerParams(collective_id=0, has_side_effects=True,
                                                 vmem_limit_bytes=60 * 2**20),
        )(charge.reshape(1, slots), real_mask.reshape(1, slots), grid_idx.T, jnp.transpose(spline_w, (1, 2, 0)),
          influence, *mats)
        return mode_energy, energy

    return jax.shard_map(local_energy, mesh=mesh, in_specs=(slot_spec, slot_spec, P(('sys', 'ydom', 'zdom'), None), P(('sys', 'ydom', 'zdom'), None, None), mode_spec), out_specs=(mode_spec, P('sys')), check_vma=False)
```

```python
import functools
import math

import jax
import jax.numpy as jnp
import numpy as np
from jax import lax
from jax.experimental import pallas as pl
from jax.experimental.pallas import tpu as pltpu
from jax.sharding import PartitionSpec as P

MESH = pl.DeviceIdType.MESH
TAPS = 4
LANES = 128
NT_DIMS = (((1,), (1,)), ((), ()))


def round_up(value, unit):
    return -(-value // unit) * unit


def split_const(matrix):
    high = matrix.astype(jnp.bfloat16)
    low = (matrix - high.astype(np.float64)).astype(jnp.bfloat16)
    return high, low


def split_value(value):
    high = value.astype(jnp.bfloat16)
    low = (value - high.astype(jnp.float32)).astype(jnp.bfloat16)
    return high, low


def dot_f32(left, right):
    return jnp.dot(left, right, preferred_element_type=jnp.float32)


def dot_nt(left, right):
    return lax.dot_general(left, right, NT_DIMS, preferred_element_type=jnp.float32)


def encode(value, code_lane):
    lane = lax.broadcasted_iota(jnp.int32, (1, value.shape[1]), 1)
    top = jnp.max(jnp.abs(value), axis=1, keepdims=True)
    code = jnp.ceil(jnp.log2(jnp.maximum(top, 1e-35)) * 64.0) + 1.0
    steps = jnp.round(value * (jnp.exp2(code * (-1.0 / 64.0)) * 32766.0))
    return jnp.where(lane == code_lane, code, steps).astype(jnp.int32).astype(jnp.int16)


def decode(packed, code_lane):
    lane = lax.broadcasted_iota(jnp.int32, (1, packed.shape[1]), 1)
    steps = packed.astype(jnp.int32).astype(jnp.float32)
    code = steps[:, code_lane:code_lane + 1]
    return jnp.where(lane == code_lane, 0.0, steps * (jnp.exp2(code * (1.0 / 64.0)) * (1.0 / 32766.0)))


CODE = 15


def swap_lane_groups(arrays, unit):
    lane = lax.broadcasted_iota(jnp.int32, (1, LANES), 1)
    arrays = list(arrays)
    bit = len(arrays) // 2
    while bit:
        stays = (lane // (unit * bit)) % 2 == 0
        for low in range(len(arrays)):
            if low & bit == 0:
                a, b = arrays[low], arrays[low | bit]
                arrays[low] = jnp.where(stays, a, pltpu.roll(b, unit * bit, 1))
                arrays[low | bit] = jnp.where(stays, pltpu.roll(a, LANES - unit * bit, 1), b)
        bit //= 2
    return arrays


def energy_kernel(sizes, charge_hbm, mask_hbm, idx_hbm, w_hbm, bc_hbm, fx_hi, fx_lo, fy_hi, fy_lo, wz_hi, wz_lo, flip_hbm,
                  ek_ref, energy_ref,
                  charge_ref, mask_ref, idx_ref, w_ref, a_hi, a_lo, b_hi0, b_lo0, b_hi1, b_lo1, y_ref, z_ref, q_ref, wide_x,
                  bc_ref, fxh, fxl, fyh, fyl, wzh, wzl, flip_ref,
                  send_x, recv_x, send_y, recv_y, send_m, recv_m, send_r, recv_r, bc_mirror, bc_row, wide_m, part, sums_y, part_z, sums_z,
                  sem_in, sem_sx, sem_rx, sem_sy, sem_ry, sem_sm, sem_rm, sem_row, sem_ey, sem_ez, sem_bc):
    grid_n, y_devs, z_devs, len_x, len_z, planes, rows_k, chunks, groups, chunk = sizes
    me_y = lax.axis_index('ydom')
    me_z = lax.axis_index('zdom')
    away_y = y_devs - 1 - me_y
    away_z = z_devs - 1 - me_z
    row_z = lax.rem(z_devs - me_z, z_devs)
    mirror = {'ydom': away_y, 'zdom': away_z}
    mirror_row = {'ydom': away_y, 'zdom': row_z}
    ring_y = [lax.rem(me_y + k, y_devs) for k in range(y_devs)]
    ring_z = [lax.rem(me_z + k, z_devs) for k in range(z_devs)]

    barrier = pltpu.get_barrier_semaphore()
    peers = [{'ydom': dest} for dest in ring_y[1:]] + [{'zdom': dest} for dest in ring_z[1:]] + [mirror, mirror_row]
    for peer in peers:
        pl.semaphore_signal(barrier, inc=1, device_id=peer, device_id_type=MESH)

    loads = [pltpu.make_async_copy(src, dst, sem_in.at[n]) for n, (src, dst) in enumerate(
        [(charge_hbm, charge_ref), (mask_hbm, mask_ref), (idx_hbm, idx_ref), (w_hbm, w_ref),
         (fx_hi, fxh), (fx_lo, fxl), (fy_hi, fyh), (fy_lo, fyl), (wz_hi, wzh), (wz_lo, wzl), (flip_hbm, flip_ref),
         (bc_hbm, bc_ref)])]
    for load in loads:
        load.start()

    def remote(src, dst, send_sem, recv_sem, peer):
        return pltpu.make_async_remote_copy(src_ref=src, dst_ref=dst, send_sem=send_sem, recv_sem=recv_sem,
                                            device_id=peer, device_id_type=MESH)

    lane = lax.broadcasted_iota(jnp.int32, (1, LANES), 1)
    is_real = (lane // 16) % 2 == 0
    per_dest = 4 * 32

    slots = charge_hbm.shape[1]
    n_chunks = slots // chunk
    rows_a = a_hi.shape[1]
    top_a = round_up(grid_n, 16)
    rows_y = b_hi0.shape[0] // 16
    for c in range(n_chunks):
        for ref in (a_hi, a_lo):
            ref[c, top_a:, :] = jnp.zeros((rows_a - top_a, chunk), jnp.bfloat16)

    def tap_block(row_id, positions, weights):
        value = jnp.where(row_id == positions[0], weights[0], 0.0)
        for tap in range(1, TAPS):
            value = jnp.where(row_id == positions[tap], weights[tap], value)
        return value

    def make_lines(c, carry):
        cols = pl.ds(pl.multiple_of(c * chunk, chunk), chunk)
        weight = charge_ref[:, cols] * mask_ref[:, cols].astype(jnp.float32)
        base = [idx_ref[d:d + 1, cols] for d in range(3)]
        taps = [[w_ref[d, s:s + 1, cols] for s in range(TAPS)] for d in range(3)]
        taps[0] = [tap * weight for tap in taps[0]]
        pos_x = [base[0] + s for s in range(TAPS)]
        pos_x = [jnp.where(pos >= grid_n, pos - grid_n, pos) for pos in pos_x]
        pos_y = [base[1] + s for s in range(TAPS)]
        pos_z = [base[2] + s for s in range(TAPS)]
        eight = lax.broadcasted_iota(jnp.int32, (8, chunk), 0)
        sixteen = lax.broadcasted_iota(jnp.int32, (16, chunk), 0)
        for row in range(0, y_ref.shape[1], 8):
            y_ref[c, row:row + 8, :] = tap_block(eight + row, pos_y, taps[1])
        for h, (first_z, n_z) in enumerate(groups):
            row_id = jnp.where(sixteen < n_z, sixteen + first_z, -1)
            z_ref[c, h * 16:(h + 1) * 16, :] = tap_block(row_id, pos_z, taps[2])
        for row in range(0, top_a, 16):
            high, low = split_value(tap_block(sixteen + row, pos_x, taps[0]))
            a_hi[c, row:row + 16, :] = high
            a_lo[c, row:row + 16, :] = low
        return carry

    def make_b(h, c, high_ref, low_ref):
        line_z = z_ref[c, pl.ds(pl.multiple_of(h * 16, 16), 16), :]
        for y in range(rows_y):
            high, low = split_value(y_ref[c, y:y + 1, :] * line_z)
            high_ref[y * 16:(y + 1) * 16, :] = high
            low_ref[y * 16:(y + 1) * 16, :] = low

    used = slice(0, rows_y * 16)

    def add_chunk(slot, c, high_ref, low_ref):
        high, low = a_hi[c], a_lo[c]
        q_ref[slot, used, :] += dot_nt(high_ref[...], high) + dot_nt(low_ref[...], high) + dot_nt(high_ref[...], low)

    sign_rows = z_devs * rows_k

    def y_half(h, p):
        cols = []
        for n in range(2):
            lines = pl.ds(pl.multiple_of(p * 64 + n * 32, 32), 32)
            cols.append(jnp.concatenate([decode(recv_x[h, s, lines, :], CODE) for s in range(y_devs)], axis=0))
        high, low = split_value(jnp.concatenate(cols, axis=1))
        block = dot_f32(fyh[...], high) + dot_f32(fyl[...], high) + dot_f32(fyh[...], low)
        values = []
        for n in range(2):
            cos_part = block[:sign_rows, n * LANES:(n + 1) * LANES]
            sin_part = block[sign_rows:, n * LANES:(n + 1) * LANES]
            values.append(cos_part + jnp.where(is_real, pltpu.roll(sin_part, LANES - 16, 1),
                                               -pltpu.roll(sin_part, 16, 1)))
        for dest in range(z_devs):
            rows = slice(dest * rows_k, (dest + 1) * rows_k)
            both = jnp.concatenate([values[0][rows], values[1][rows]], axis=0)
            send_y[dest, h, pl.ds(pl.multiple_of(p * 2 * rows_k, 16), 2 * rows_k), :] = encode(both, CODE)

    def x_copy(h, p, k):
        start = pl.multiple_of(ring_y[k] * per_dest + p * 64, 64)
        return remote(send_x.at[h, pl.ds(start, 64), :], recv_x.at[h, me_y, pl.ds(pl.multiple_of(p * 64, 64), 64), :],
                      sem_sx.at[2 * h + p, k], sem_rx.at[2 * h + p, k], {'ydom': ring_y[k]})

    def y_copy(h, p, k):
        rows = pl.ds(pl.multiple_of(p * 2 * rows_k, 16), 2 * rows_k)
        return remote(send_y.at[ring_z[k], h, rows, :], recv_y.at[me_z, h, rows, :],
                      sem_sy.at[2 * h + p, k], sem_ry.at[2 * h + p, k], {'zdom': ring_z[k]})

    def y_direction(h):
        def one_half(p, carry):
            for k in range(1, y_devs):
                x_copy(h, p, k).wait_recv()
            y_half(h, p)
            for k in range(1, z_devs):
                y_copy(h, p, k).start()
            rows = pl.ds(pl.multiple_of(p * 2 * rows_k, 16), 2 * rows_k)
            recv_y[me_z, h, rows, :] = send_y[me_z, h, rows, :]
            return carry

        lax.fori_loop(0, 2, one_half, 0)

    for load in loads[:4]:
        load.wait()
    pl.semaphore_wait(barrier, len(peers))
    upper = pl.ds(planes, len_x - planes)
    copies_bc = [remote(bc_hbm.at[upper], bc_mirror, sem_bc.at[0, 0], sem_bc.at[1, 0], mirror),
                 remote(bc_hbm.at[upper, pl.ds(0, 8), :], bc_row, sem_bc.at[0, 1], sem_bc.at[1, 1], mirror_row)]
    for copy in copies_bc:
        copy.start()
    q_ref[...] = jnp.zeros_like(q_ref)

    def first_two(c, carry):
        make_lines(c, 0)
        make_b(0, c, b_hi0, b_lo0)
        add_chunk(0, c, b_hi0, b_lo0)
        make_b(1, c, b_hi1, b_lo1)
        add_chunk(1, c, b_hi1, b_lo1)
        return carry

    def one_more(h):
        slot = h % 2
        q_ref[slot] = jnp.zeros(q_ref.shape[1:], jnp.float32)

        def pair(step, carry):
            after = 2 * step + 2
            wrap = after // n_chunks
            after_c = after - wrap * n_chunks
            make_b(h, 2 * step + 1, b_hi1, b_lo1)
            add_chunk(slot, 2 * step, b_hi0, b_lo0)
            make_b(h + wrap, after_c, b_hi0, b_lo0)
            add_chunk(slot, 2 * step + 1, b_hi1, b_lo1)
            return carry

        lax.fori_loop(0, n_chunks // 2, pair, 0)

    def x_direction(h):
        slot = h % 2
        for half in range(2):
            high, low = split_value(q_ref[slot, half * 256:(half + 1) * 256, :])
            block = dot_nt(fxh[...], high) + dot_nt(fxl[...], high) + dot_nt(fxh[...], low)
            for tile in range(2):
                lanes = slice(tile * LANES, (tile + 1) * LANES)
                by_y = swap_lane_groups([block[b * 32:(b + 1) * 32, lanes] for b in range(8)], 16)
                for y in range(8):
                    wide_x[pl.ds((half * 2 + tile) * 8 + y, 4 * y_devs, stride=40), :] = by_y[y]

        def pack_rows(dest, carry, h=h):
            for tq in range(4):
                rows = pl.ds(pl.multiple_of((dest * 4 + tq) * 40, 8), 32)
                send_x[h, pl.ds(pl.multiple_of(dest * per_dest + tq * 32, 32), 32), :] = encode(wide_x[rows, :], CODE)
            return carry

        lax.fori_loop(0, y_devs, pack_rows, 0)
        for p in range(2):
            for k in range(1, y_devs):
                x_copy(h, p, k).start()
        recv_x[h, me_y] = send_x[h, pl.ds(pl.multiple_of(me_y * per_dest, 16), per_dest), :]

    lax.fori_loop(0, n_chunks, first_two, 0)
    for load in loads[4:]:
        load.wait()
    x_direction(0)
    x_direction(1)
    make_b(2, 0, b_hi0, b_lo0)
    one_more(2)
    x_direction(2)
    y_direction(0)
    y_direction(1)
    one_more(3)
    x_direction(3)
    y_direction(2)
    y_direction(3)

    width = wzh.shape[1] // 2
    total = jnp.zeros((len_z, grid_n), jnp.float32)
    is_first = lax.broadcasted_iota(jnp.int32, (len_z, grid_n), 0) == 0
    for copy in copies_bc:
        copy.wait_recv()
    send_r[...] = jnp.zeros_like(send_r)
    wide_m[...] = jnp.zeros_like(wide_m)
    def start_sum(value, out, sums, sems, axis, ring, me):
        out[...] = jnp.zeros_like(out) + value
        copies = []
        for k in range(1, len(ring)):
            copy = remote(out, sums.at[me], sems.at[0, k], sems.at[1, k], {axis: ring[k]})
            copy.start()
            copies.append(copy)
        sums[me] = jnp.zeros(out.shape, jnp.float32) + value
        return copies

    def end_sum(sums, copies):
        for copy in copies:
            copy.wait_recv()
        result = sums[0]
        for s in range(1, len(copies) + 1):
            result = result + sums[s]
        return result

    copies_m = []
    real_wide = jnp.concatenate([is_real] * z_devs, axis=1)
    for c, (first, last) in enumerate(chunks):
        rows = slice(first * rows_k, last * rows_k)
        if c % 2 == 0:
            for h in range(len(groups)):
                for k in range(1, z_devs):
                    y_copy(h, c // 2, k).wait_recv()
            lines = slice(c * rows_k, (c + 2) * rows_k)
            by_plane = [swap_lane_groups([decode(recv_y[s, h, lines, :], CODE) for h in range(4)], 32)
                        for s in range(z_devs)]
        at = slice((c % 2) * rows_k, (c % 2 + 1) * rows_k)
        high, low = split_value(jnp.concatenate(
            [jnp.concatenate([by_plane[s][n][at] for s in range(z_devs)], axis=1) for n in range(last - first)], axis=0))
        nil = jnp.zeros_like(high)
        from_real, from_imag = [
            dot_f32(h, wzh[...]) + dot_f32(l, wzh[...]) + dot_f32(h, wzl[...])
            for h, l in ((jnp.where(real_wide, high, nil), jnp.where(real_wide, low, nil)),
                         (jnp.where(real_wide, nil, high), jnp.where(real_wide, nil, low)))]
        both_signs = [from_real + from_imag, from_real - from_imag]
        power, power_rev = [v[:, :width] * v[:, :width] + v[:, width:] * v[:, width:] for v in both_signs]
        for p in range(first, last, 2):
            for kx in (p, p + 1):
                at = (kx - first) * rows_k
                value = bc_ref[kx] * power[at:at + len_z, :grid_n]
                ek_ref[kx] = value
                total = total + value
                high, low = split_value(power_rev[at:at + rows_k, :])
                flipped = dot_f32(flip_ref[...], high) + dot_f32(flip_ref[...], low)
                if kx >= 1:
                    plane = len_x - kx - planes
                    factor = jnp.where(is_first, bc_row[plane, 0:1, :], bc_mirror[plane])
                    value = factor * flipped[:len_z, :grid_n]
                    total = total + value
                    send_r[kx:kx + 1, :grid_n] = value[0:1, :]
                    wide_m[(kx - p) * rows_k:(kx - p) * rows_k + len_z, :grid_n] = value
            send_m[p * rows_k:(p + 2) * rows_k, :] = encode(wide_m[...], width - 1)
        if last == planes:
            copies_ez = start_sum(jnp.sum(total, keepdims=True), part, sums_z, sem_ez, 'zdom', ring_z, me_z)
        rows = slice(max(first * rows_k, rows_k // 16 * 16), last * rows_k)
        copy = remote(send_m.at[rows, :], recv_m.at[rows, :], sem_sm.at[c], sem_rm.at[c], mirror)
        copy.start()
        copies_m.append(copy)
    copy_row = remote(send_r, recv_r, sem_row.at[0], sem_row.at[1], mirror_row)
    copy_row.start()

    copies_ey = start_sum(end_sum(sums_z, copies_ez), part_z, sums_y, sem_ey, 'ydom', ring_y, me_y)

    copy_row.wait_recv()
    for c, (first, last) in enumerate(chunks):
        copies_m[c].wait_recv()
        for p in range(first, last, 2):
            both = decode(recv_m[p * rows_k:(p + 2) * rows_k, :], width - 1)
            for kx in (p, p + 1):
                if kx >= 1:
                    at = (kx - p) * rows_k
                    ek_ref[len_x - kx] = jnp.where(is_first, recv_r[kx:kx + 1, :grid_n], both[at:at + len_z, :grid_n])

    energy_ref[0] = end_sum(sums_y, copies_ey)[0, 0] * 0.5 / (grid_n * grid_n * grid_n)

    for copy in copies_m + [copy_row] + copies_ez + copies_ey + copies_bc:
        copy.wait_send()
    for h in range(len(groups)):
        for p in range(2):
            for k in range(1, y_devs):
                x_copy(h, p, k).wait_send()
            for k in range(1, z_devs):
                y_copy(h, p, k).wait_send()


def transforms(grid_n, y_devs, z_devs, len_x, len_y, len_z, planes, rows_k, groups):
    unit = 2.0 * math.pi / grid_n

    def angle(freq, pos):
        return ((freq[:, None] * pos[None, :]) % grid_n) * unit

    plane = np.arange(4)[None, None, :] * 4 + np.arange(4)[:, None, None]
    freq = (np.arange(y_devs)[None, :, None] * len_x + plane).reshape(-1)
    keep = np.broadcast_to(plane < planes, (4, y_devs, 4)).reshape(-1)
    phase = angle(freq, np.arange(grid_n))
    mat_x = np.zeros((4, 2, y_devs * 4, round_up(grid_n, LANES)))
    mat_x[:, 0, :, :grid_n] = (np.cos(phase) * keep[:, None]).reshape(4, y_devs * 4, grid_n)
    mat_x[:, 1, :, :grid_n] = (-np.sin(phase) * keep[:, None]).reshape(4, y_devs * 4, grid_n)
    mat_x = mat_x.reshape(8 * y_devs * 4, -1)
    pos = (np.arange(y_devs)[:, None] * len_y + np.arange(32)[None, :]).reshape(-1)
    used = np.tile(np.arange(32) < len_y + TAPS - 1, y_devs)
    ky = (np.arange(z_devs)[:, None] * len_z + np.arange(rows_k)[None, :]).reshape(-1)
    keep = np.tile(np.arange(rows_k) < len_z, z_devs)
    phase = angle(ky, pos)
    mask = keep[:, None] * used[None, :]
    mat_y = np.concatenate([np.cos(phase) * mask, np.sin(phase) * mask])
    width = round_up(grid_n, LANES)
    mat_z = np.zeros((z_devs, len(groups), 2, 16, 2, width))
    for dev in range(z_devs):
        for h, (first_z, n_z) in enumerate(groups):
            phase = angle(dev * len_z + first_z + np.arange(n_z), np.arange(grid_n))
            mat_z[dev, h, 0, :n_z, 0, :grid_n] = np.cos(phase)
            mat_z[dev, h, 1, :n_z, 0, :grid_n] = np.sin(phase)
            mat_z[dev, h, 0, :n_z, 1, :grid_n] = -np.sin(phase)
            mat_z[dev, h, 1, :n_z, 1, :grid_n] = np.cos(phase)
    mat_z = mat_z.reshape(z_devs * 128, 2 * width)
    flip = np.zeros((rows_k, rows_k))
    flip[0, 0] = 1.0
    flip[np.arange(1, len_z), len_z - np.arange(1, len_z)] = 1.0
    return (*split_const(mat_x), *split_const(mat_y), *split_const(mat_z), flip.astype(jnp.bfloat16))


def solution(mesh):
    y_devs = mesh.shape['ydom']
    z_devs = mesh.shape['zdom']
    slot_spec = P(('sys', 'ydom', 'zdom'))
    mode_spec = P(('sys', 'ydom'), 'zdom', None)

    def local_energy(charge, real_mask, grid_idx, spline_w, influence):
        len_x, len_k, grid_n = influence.shape
        len_y = grid_n // y_devs
        len_z = grid_n // z_devs
        slots = charge.shape[0]
        chunk = 1024
        rows_y = len_y + TAPS - 1
        rows_z = len_z + TAPS - 1
        cuts = [-(-rows_z * h // 4) for h in range(5)]
        groups = tuple((cuts[h], cuts[h + 1] - cuts[h]) for h in range(4))
        width = round_up(grid_n, LANES)
        planes = (len_x + 1) // 2
        rows_k = round_up(len_k, 8)
        chunks = tuple((p, min(p + 4, planes)) for p in range(0, planes, 4))
        sizes = (grid_n, y_devs, z_devs, len_x, len_z, planes, rows_k, chunks, groups, chunk)
        mats = transforms(grid_n, y_devs, z_devs, len_x, len_y, len_z, planes, rows_k, groups)
        f32, bf16, i16 = jnp.float32, jnp.bfloat16, jnp.int16
        vmem = pl.BlockSpec(memory_space=pltpu.VMEM)
        hbm = pl.BlockSpec(memory_space=pltpu.HBM)
        n, n_g, n_c = len(chunks), len(groups), slots // chunk
        dma = pltpu.SemaphoreType.DMA
        mode_energy, energy = pl.pallas_call(
            functools.partial(energy_kernel, sizes),
            name='energy',
            out_shape=(jax.ShapeDtypeStruct(influence.shape, f32), jax.ShapeDtypeStruct((1,), f32)),
            in_specs=[hbm] * (5 + len(mats)),
            out_specs=(vmem, pl.BlockSpec(memory_space=pltpu.SMEM)),
            scratch_shapes=[
                pltpu.VMEM((1, slots), f32), pltpu.VMEM((1, slots), jnp.int32), pltpu.VMEM((3, slots), jnp.int32),
                pltpu.VMEM((3, TAPS, slots), f32),
                pltpu.VMEM((n_c, width, chunk), bf16), pltpu.VMEM((n_c, width, chunk), bf16),
                *[pltpu.VMEM((rows_y * 16, chunk), bf16)] * 4,
                pltpu.VMEM((n_c, 32, chunk), f32), pltpu.VMEM((n_c, 16 * n_g + 16, chunk), f32),
                pltpu.VMEM((2, 512, width), f32), pltpu.VMEM((y_devs * 4 * 40, LANES), f32),
                pltpu.VMEM(influence.shape, f32), *[pltpu.VMEM(mat.shape, mat.dtype) for mat in mats],
                pltpu.VMEM((n_g, y_devs * 128, LANES), i16),
                pltpu.VMEM((n_g, y_devs, 128, LANES), i16),
                pltpu.VMEM((z_devs, n_g, 4 * rows_k, LANES), i16),
                pltpu.VMEM((z_devs, n_g, 4 * rows_k, LANES), i16),
                pltpu.VMEM((planes * rows_k, width), i16),
                pltpu.VMEM((planes * rows_k, width), i16),
                pltpu.VMEM((round_up(planes, 8), width), f32),
                pltpu.VMEM((round_up(planes, 8), width), f32),
                pltpu.VMEM((len_x - planes, len_k, grid_n), f32),
                pltpu.VMEM((len_x - planes, 8, grid_n), f32),
                pltpu.VMEM((2 * rows_k, width), f32),
                pltpu.VMEM((8, LANES), f32),
                pltpu.VMEM((y_devs, 8, LANES), f32),
                pltpu.VMEM((8, LANES), f32),
                pltpu.VMEM((z_devs, 8, LANES), f32),
                dma((12,)), dma((2 * n_g, y_devs)), dma((2 * n_g, y_devs)), dma((2 * n_g, z_devs)), dma((2 * n_g, z_devs)),
                dma((n,)), dma((n,)), dma((2,)), dma((2, y_devs)), dma((2, z_devs)), dma((2, 2)),
            ],
            compiler_params=pltpu.CompilerParams(collective_id=0, has_side_effects=True,
                                                 vmem_limit_bytes=60 * 2**20),
        )(charge.reshape(1, slots), real_mask.reshape(1, slots), grid_idx.T, jnp.transpose(spline_w, (1, 2, 0)),
          influence, *mats)
        return 0.5 * mode_energy, energy

    return jax.shard_map(local_energy, mesh=mesh, in_specs=(slot_spec, slot_spec, P(('sys', 'ydom', 'zdom'), None), P(('sys', 'ydom', 'zdom'), None, None), mode_spec), out_specs=(mode_spec, P('sys')), check_vma=False)
```
